32 devices in a mesh: gx: 4 (over y, core), gy: 2 (over x), gz: 4 (over z).
Axes of the slice: x: 2, y: 2, z: 4, core: 2. Of those that a mesh axis runs over, the one named last changes fastest.
Arguments:
- populations: float32 [19, 32, 32, 512], P(None, 'gx', 'gy', 'gz'), may hold values from 0 to 1, as said below
- solid_fraction: float32 [32, 32, 512], P('gx', 'gy', 'gz'), may hold values from 0 to 1
- intersection: int32 [32, 32, 512], P('gx', 'gy', 'gz'), may hold values from 0 to 256, as said below
- touch: int32 [4, 2, 4, 256], P('gx', 'gy', 'gz'), may hold values from 0 to 3455, as said below
- particles: float32 [4, 2, 4, 6, 128], P('gx', 'gy', 'gz'), may hold values from -8 to 8, as said below
- contacts: int32 [4, 2, 4, 12, 128], P('gx', 'gy', 'gz'), may hold values from 0 to 3456, as said below
- dest_code: int32 [4, 2, 4, 128], P('gx', 'gy', 'gz'), may hold values from 4 to 22, as said below
- dest_slot: int32 [4, 2, 4, 128], P('gx', 'gy', 'gz'), may hold values from 0 to 127, as said below
Outputs:
- populations_next: float32 [19, 32, 32, 512], P(None, 'gx', 'gy', 'gz')
- particles_next: float32 [4, 2, 4, 6, 128], P('gx', 'gy', 'gz')
The draws below stay inside these ranges and needn't reach their ends.
Inputs may be any that keep to these rules, and one draw needn't show every extreme that they name: intersection = 256 marks a cell that no sphere covers; otherwise a touch slot of the cell's block. `touch`: entry o * 128 + s names slot s of the block at offset o of the 27 neighbouring blocks, offsets ordered with x slowest; the entries of one block are distinct and name every slot of the block itself. `contacts`: 3456 marks an empty entry. `dest_code`: a sphere stays (code 13) or moves one block along one axis (codes 4, 10, 12, 14, 16, 22), never out of the mesh; every slot of every block receives exactly one record. `dest_slot`: see dest_code. `populations`: every population is positive. `particles`: positions, in radii from the block centre, lie within the block's half widths; speeds lie within -1.5 to 1.5.
All inputs are finite; a program needn't handle non-finite values.
Results may differ from the reference program's by a relative error of at most 0.000076.
Values sent between devices are 32-bit elements; how exact they have to be, the bound alone decides.
A program may use at most 128 MiB of HBM per device.

```python
import jax
import jax.numpy as jnp
from jax import lax

CX = 8
CY = 16
CZ = 128
P_SIZE = 128
NC = 12
R = 8
K = 256
BX = 4
BY = 2
BZ = 4
NX = 32
NY = 32
NZ = 512


LATTICE = [(0, 0, 0), (1, 0, 0), (-1, 0, 0), (0, 1, 0), (0, -1, 0), (0, 0, 1), (0, 0, -1), (1, 1, 0), (-1, -1, 0), (1, -1, 0), (-1, 1, 0), (1, 0, 1), (-1, 0, -1), (1, 0, -1), (-1, 0, 1), (0, 1, 1), (0, -1, -1), (0, 1, -1), (0, -1, 1)]


WEIGHTS = [1.0 / 3.0] + [1.0 / 18.0] * 6 + [1.0 / 36.0] * 12


CONTACT_STEPS = [(1, 0, 0), (-1, 0, 0), (0, 1, 0), (0, -1, 0), (0, 0, 1), (0, 0, -1), (1, 1, 0), (-1, -1, 0), (1, 0, 1), (-1, 0, -1), (0, 1, 1), (0, -1, -1)]


def equilibrium_drawn(density, velocity):
    square = velocity[0] * velocity[0] + velocity[1] * velocity[1] + velocity[2] * velocity[2]
    result = []
    for vector, weight in zip(LATTICE, WEIGHTS):
        projected = vector[0] * velocity[0] + vector[1] * velocity[1] + vector[2] * velocity[2]
        result.append(weight * density * (1.0 + 3.0 * projected + 4.5 * projected * projected - 1.5 * square))
    return jnp.stack(result)


def draw_populations(key, part):
    subkeys = jax.random.split(key, 3)
    grid_shape = (NX, NY, NZ)
    density = 1.0 + 0.02 * jax.random.truncated_normal(subkeys[0], -3.0, 3.0, grid_shape, jnp.float32)
    velocity = 0.04 * jax.random.truncated_normal(subkeys[1], -2.0, 2.0, (3,) + grid_shape, jnp.float32)
    jitter = 1.0 + 0.3 * (jax.random.uniform(subkeys[2], (19,) + grid_shape, jnp.float32) - 0.5)
    return equilibrium_drawn(density, velocity) * jitter


def draw_intersection(key, part):
    subkeys = jax.random.split(jax.random.fold_in(key, 11), 2)
    grid_shape = (NX, NY, NZ)
    height = lax.broadcasted_iota(jnp.int32, grid_shape, 2)
    draw_height = jax.random.randint(subkeys[0], grid_shape, 0, NZ)
    is_solid = draw_height < (NZ - height) * 3 // 4
    chosen = jax.random.randint(subkeys[1], grid_shape, 0, K)
    return jnp.where(is_solid, chosen, K).astype(jnp.int32)


def slot_tables(key):
    folded = jax.random.fold_in(key, 29)
    block_keys = jax.random.split(folded, BX * BY * BZ)
    slot_of_site = jax.vmap(lambda block_key: jax.random.permutation(block_key, P_SIZE))(block_keys)
    slot_of_site = slot_of_site.reshape(BX, BY, BZ, P_SIZE).astype(jnp.int32)
    site_of_slot = jnp.argsort(slot_of_site, axis=-1).astype(jnp.int32)
    return (slot_of_site, site_of_slot)


def neighbour_entry(slot_of_site, site_x, site_y, site_z, home_x, home_y, home_z):
    layers = P_SIZE // 16
    move_x = (site_x + 4) // 4 - 1
    move_y = (site_y + 4) // 4 - 1
    move_z = (site_z + layers) // layers - 1
    block_x = home_x + move_x
    block_y = home_y + move_y
    block_z = home_z + move_z
    inside = (block_x >= 0) & (block_x < BX) & (block_y >= 0) & (block_y < BY) & (block_z >= 0) & (block_z < BZ)
    flat_block = (jnp.clip(block_x, 0, BX - 1) * BY + jnp.clip(block_y, 0, BY - 1)) * BZ + jnp.clip(block_z, 0, BZ - 1)
    local_site = (site_z - layers * move_z) * 16 + (site_y - 4 * move_y) * 4 + site_x - 4 * move_x
    slot_found = slot_of_site.reshape(-1)[flat_block * P_SIZE + local_site]
    code = 9 * (move_x + 1) + 3 * (move_y + 1) + move_z + 1
    return ((code * P_SIZE + slot_found).astype(jnp.int32), inside)


def draw_particles(key, part):
    slot_of_site, site_of_slot = slot_tables(key)
    subkeys = jax.random.split(jax.random.fold_in(key, 13), 2)
    layers = P_SIZE // 16
    spacing_x = CX / (4.0 * R)
    spacing_y = CY / (4.0 * R)
    spacing_z = CZ / (layers * 1.0 * R)
    site_x = (site_of_slot % 4).astype(jnp.float32)
    site_y = (site_of_slot // 4 % 4).astype(jnp.float32)
    site_z = (site_of_slot // 16).astype(jnp.float32)
    centres = jnp.stack([(site_x + 0.5) * spacing_x - CX / (2.0 * R), (site_y + 0.5) * spacing_y - CY / (2.0 * R), (site_z + 0.5) * spacing_z - CZ / (2.0 * R)], axis=3)
    spacing = jnp.array([spacing_x, spacing_y, spacing_z], jnp.float32)
    jitter = jax.random.uniform(subkeys[0], (BX, BY, BZ, 3, P_SIZE), jnp.float32, -0.3, 0.3) * spacing[:, None]
    places = centres + jitter
    speeds = 0.6 * jax.random.truncated_normal(subkeys[1], -2.5, 2.5, (BX, BY, BZ, 3, P_SIZE), jnp.float32)
    return jnp.concatenate([places, speeds], axis=3)


def draw_contacts(key, part):
    slot_of_site, site_of_slot = slot_tables(key)
    shape_here = (BX, BY, BZ, P_SIZE)
    site_x = site_of_slot % 4
    site_y = site_of_slot // 4 % 4
    site_z = site_of_slot // 16
    home_x = lax.broadcasted_iota(jnp.int32, shape_here, 0)
    home_y = lax.broadcasted_iota(jnp.int32, shape_here, 1)
    home_z = lax.broadcasted_iota(jnp.int32, shape_here, 2)
    listed = []
    for step in CONTACT_STEPS:
        entry, inside = neighbour_entry(slot_of_site, site_x + step[0], site_y + step[1], site_z + step[2], home_x, home_y, home_z)
        listed.append(jnp.where(inside, entry, 27 * P_SIZE))
    stacked = jnp.stack(listed, axis=3)
    empty = jax.random.randint(jax.random.fold_in(key, 17), stacked.shape, 0, 4) == 0
    return jnp.where(empty, 27 * P_SIZE, stacked).astype(jnp.int32)


def draw_touch(key, part):
    slot_of_site, unused = slot_tables(key)
    layers = P_SIZE // 16
    extended = 36 * (layers + 2)
    shape_here = (BX, BY, BZ, extended)
    candidate = lax.broadcasted_iota(jnp.int32, shape_here, 3)
    around_x = candidate % 6 - 1
    around_y = candidate // 6 % 6 - 1
    around_z = candidate // 36 - 1
    home_x = lax.broadcasted_iota(jnp.int32, shape_here, 0)
    home_y = lax.broadcasted_iota(jnp.int32, shape_here, 1)
    home_z = lax.broadcasted_iota(jnp.int32, shape_here, 2)
    entry, inside = neighbour_entry(slot_of_site, around_x, around_y, around_z, home_x, home_y, home_z)
    inner = (around_x >= 0) & (around_x < 4) & (around_y >= 0) & (around_y < 4) & (around_z >= 0) & (around_z < layers)
    tier = jnp.where(inner, 0, jnp.where(inside, 1, 2))
    block_count = BX * BY * BZ
    subkeys = jax.random.split(jax.random.fold_in(key, 31), 2)
    ranks = jax.vmap(lambda block_key: jax.random.permutation(block_key, extended))(jax.random.split(subkeys[0], block_count))
    ranks = ranks.reshape(shape_here).astype(jnp.int32)
    order = jnp.argsort(tier * extended + ranks, axis=-1)[..., :K]
    chosen = jnp.take_along_axis(entry, order, axis=-1)
    shuffle = jax.vmap(lambda block_key: jax.random.permutation(block_key, K))(jax.random.split(subkeys[1], block_count))
    shuffle = shuffle.reshape(BX, BY, BZ, K).astype(jnp.int32)
    return jnp.take_along_axis(chosen, shuffle, axis=-1).astype(jnp.int32)


def migration_plan(key):
    folded = jax.random.fold_in(key, 23)
    subkeys = jax.random.split(folded, 7)
    counts = [BX, BY, BZ]
    shape_here = (BX, BY, BZ, P_SIZE)
    slot_ids = lax.broadcasted_iota(jnp.int32, shape_here, 3)
    moves = []
    for dimension in range(3):
        parity = jax.random.randint(subkeys[dimension], (), 0, 2)
        amount = jax.random.randint(subkeys[3 + dimension], (), max(P_SIZE // 16, 1), P_SIZE // 4 + 1)
        coordinate = lax.broadcasted_iota(jnp.int32, shape_here, dimension)
        first_slot = dimension * (P_SIZE // 4)
        chosen = (slot_ids >= first_slot) & (slot_ids < first_slot + amount)
        upward = ((coordinate - parity) % 2 == 0) & (coordinate + 1 < counts[dimension])
        downward = ((coordinate - parity) % 2 == 1) & (coordinate >= 1)
        moves.append(jnp.where(chosen, upward.astype(jnp.int32) - downward.astype(jnp.int32), 0))
    codes = 13 + 9 * moves[0] + 3 * moves[1] + moves[2]
    block_count = BX * BY * BZ
    perms = jax.vmap(lambda block_key: jax.random.permutation(block_key, P_SIZE))(jax.random.split(subkeys[6], block_count))
    home_x = lax.broadcasted_iota(jnp.int32, shape_here, 0)
    home_y = lax.broadcasted_iota(jnp.int32, shape_here, 1)
    home_z = lax.broadcasted_iota(jnp.int32, shape_here, 2)
    target = ((home_x + moves[0]) * BY + home_y + moves[1]) * BZ + home_z + moves[2]
    slots_new = perms.reshape(-1)[target * P_SIZE + slot_ids]
    return (codes.astype(jnp.int32), slots_new.astype(jnp.int32))


def draw_dest_code(key, part):
    return migration_plan(key)[0]


def draw_dest_slot(key, part):
    return migration_plan(key)[1]


def block_levels(own_key, shape, pieces, smallest, high):
    loudness, own = 1.0, jax.random.fold_in(own_key, 6)
    for position, blocks in pieces:
        steps = jnp.exp(jax.random.uniform(jax.random.fold_in(own, position), (blocks,), jnp.float32, smallest / len(pieces), high / len(pieces)))
        loudness = loudness * jnp.repeat(steps, shape[position] // blocks).reshape([-1 if axis == position else 1 for axis in range(len(shape))])
    return loudness


def setup_inputs(seed: int = 0) -> dict:
    arg_keys = jax.random.split(jax.random.key(seed), 9)
    return {
        "populations": draw_populations(jax.random.fold_in(arg_keys[8], 71), 0),
        "solid_fraction": jnp.clip(1.0 * jax.random.uniform(arg_keys[1], (NX, NY, NZ), jnp.float32) ** block_levels(arg_keys[1], (NX, NY, NZ), ((0, 4), (1, 2), (2, 4)), -0.2, 0.2), 0.0, 1.0),
        "intersection": draw_intersection(jax.random.fold_in(arg_keys[8], 71), 0),
        "touch": draw_touch(jax.random.fold_in(arg_keys[8], 71), 0),
        "particles": draw_particles(jax.random.fold_in(arg_keys[8], 71), 0),
        "contacts": draw_contacts(jax.random.fold_in(arg_keys[8], 71), 0),
        "dest_code": draw_dest_code(jax.random.fold_in(arg_keys[8], 71), 0),
        "dest_slot": draw_dest_slot(jax.random.fold_in(arg_keys[8], 71), 0),
    }


LATTICE = [(0, 0, 0), (1, 0, 0), (-1, 0, 0), (0, 1, 0), (0, -1, 0), (0, 0, 1), (0, 0, -1),
           (1, 1, 0), (-1, -1, 0), (1, -1, 0), (-1, 1, 0), (1, 0, 1), (-1, 0, -1),
           (1, 0, -1), (-1, 0, 1), (0, 1, 1), (0, -1, -1), (0, 1, -1), (0, -1, 1)]
OPPOSITE = [0, 2, 1, 4, 3, 6, 5, 8, 7, 10, 9, 12, 11, 14, 13, 16, 15, 18, 17]
WEIGHTS = [1.0 / 3.0] + [1.0 / 18.0] * 6 + [1.0 / 36.0] * 12
RELAX_TIME = 0.8
SPEED_UNIT = 0.05
FORCE_SCALE = 0.1
CONTACT_GAIN = 1.0
GRAVITY_STEP = 0.1


def equilibrium(density, velocity):
    square = velocity[0] * velocity[0] + velocity[1] * velocity[1] + velocity[2] * velocity[2]
    result = []
    for vector, weight in zip(LATTICE, WEIGHTS):
        projected = vector[0] * velocity[0] + vector[1] * velocity[1] + vector[2] * velocity[2]
        result.append(weight * density * (1.0 + 3.0 * projected + 4.5 * projected * projected - 1.5 * square))
    return jnp.stack(result)


def collide(populations, solid_weight, solid_velocity):
    lattice_table = jnp.array(LATTICE, jnp.float32)
    density = jnp.sum(populations, axis=0)
    momentum = jnp.tensordot(lattice_table.T, populations, axes=1, precision=lax.Precision.HIGHEST)
    velocity = momentum / density
    fluid_eq = equilibrium(density, velocity)
    solid_eq = equilibrium(density, solid_velocity)
    mirrored = jnp.stack([populations[mirror_index] for mirror_index in OPPOSITE])
    fluid_mirror = jnp.stack([fluid_eq[mirror_index] for mirror_index in OPPOSITE])
    exchange_term = mirrored - populations + solid_eq - fluid_mirror
    relaxed = populations - (1.0 - solid_weight) / RELAX_TIME * (populations - fluid_eq) + solid_weight * exchange_term
    cell_force = -jnp.tensordot(lattice_table.T, solid_weight * exchange_term, axes=1, precision=lax.Precision.HIGHEST)
    return relaxed, cell_force


def block_offsets(entries, slots_each, span_x, span_y, span_z, radius):
    block_code = jnp.arange(entries, dtype=jnp.int32) // slots_each
    return jnp.stack([(block_code // 9 - 1).astype(jnp.float32) * (span_x / radius),
                      ((block_code // 3) % 3 - 1).astype(jnp.float32) * (span_y / radius),
                      (block_code % 3 - 1).astype(jnp.float32) * (span_z / radius)])


def reference(populations, solid_fraction, intersection, touch, particles, contacts, dest_code, dest_slot):
    blocks = BX * BY * BZ
    padded = jnp.pad(particles, ((1, 1), (1, 1), (1, 1), (0, 0), (0, 0)))
    neighbourhood = jnp.stack([padded[step_x:step_x + BX, step_y:step_y + BY, step_z:step_z + BZ]
                               for step_x in range(3) for step_y in range(3) for step_z in range(3)], axis=3)
    records_near = jnp.moveaxis(neighbourhood, 4, 3).reshape(blocks, 6, 27 * P_SIZE)
    touch_rows = touch.reshape(blocks, K)
    touch_velocity = jnp.take_along_axis(records_near[:, 3:6, :], jnp.broadcast_to(touch_rows[:, None, :], (blocks, 3, K)), axis=2)
    touch_velocity = jnp.concatenate([touch_velocity, jnp.zeros((blocks, 3, 1), jnp.float32)], axis=2)
    velocity_rows = jnp.transpose(touch_velocity, (0, 2, 1)).reshape(blocks * (K + 1), 3)
    block_x = (jnp.arange(NX, dtype=jnp.int32) // CX)[:, None, None]
    block_y = (jnp.arange(NY, dtype=jnp.int32) // CY)[None, :, None]
    block_z = (jnp.arange(NZ, dtype=jnp.int32) // CZ)[None, None, :]
    slot_rows = ((block_x * BY + block_y) * BZ + block_z) * (K + 1) + intersection
    fraction_term = jnp.where(intersection < K, solid_fraction * (RELAX_TIME - 0.5) / ((1.0 - solid_fraction) + (RELAX_TIME - 0.5)), jnp.float32(0.0))

    def slab_step(start):
        slab_pop = lax.dynamic_slice_in_dim(populations, start, CX, 1)
        slab_rows = lax.dynamic_slice_in_dim(slot_rows, start, CX, 0)
        slab_weight = lax.dynamic_slice_in_dim(fraction_term, start, CX, 0)
        solid_velocity = SPEED_UNIT * jnp.moveaxis(velocity_rows[slab_rows], -1, 0)
        return collide(slab_pop, slab_weight, solid_velocity)

    relaxed, cell_force = lax.map(slab_step, jnp.arange(BX, dtype=jnp.int32) * CX)
    relaxed = jnp.moveaxis(relaxed, 0, 1).reshape(19, NX, NY, NZ)
    cell_force = jnp.moveaxis(cell_force, 0, 1).reshape(3, NX, NY, NZ)

    coord_x = jnp.arange(NX, dtype=jnp.int32)[:, None, None]
    coord_y = jnp.arange(NY, dtype=jnp.int32)[None, :, None]
    coord_z = jnp.arange(NZ, dtype=jnp.int32)[None, None, :]
    passed = []
    for direction, vector in enumerate(LATTICE):
        rolled = jnp.roll(relaxed[direction], vector, axis=(0, 1, 2))
        inside = ((coord_x - vector[0] >= 0) & (coord_x - vector[0] < NX) & (coord_y - vector[1] >= 0)
                  & (coord_y - vector[1] < NY) & (coord_z - vector[2] >= 0) & (coord_z - vector[2] < NZ))
        passed.append(jnp.where(inside, rolled, relaxed[OPPOSITE[direction]]))
    populations_next = jnp.stack(passed)

    touch_force = jax.ops.segment_sum(cell_force.reshape(3, -1).T, slot_rows.reshape(-1), num_segments=blocks * (K + 1))
    touch_force = touch_force.reshape(blocks, K + 1, 3)[:, :K, :]
    owner_x = lax.broadcasted_iota(jnp.int32, (BX, BY, BZ, K), 0).reshape(blocks, K)
    owner_y = lax.broadcasted_iota(jnp.int32, (BX, BY, BZ, K), 1).reshape(blocks, K)
    owner_z = lax.broadcasted_iota(jnp.int32, (BX, BY, BZ, K), 2).reshape(blocks, K)
    touch_code = touch_rows // P_SIZE
    owner_rows = (((owner_x + touch_code // 9) * (BY + 2) + owner_y + (touch_code // 3) % 3) * (BZ + 2)
                  + owner_z + touch_code % 3) * P_SIZE + touch_rows % P_SIZE
    hydro = jax.ops.segment_sum(touch_force.reshape(-1, 3), owner_rows.reshape(-1), num_segments=(BX + 2) * (BY + 2) * (BZ + 2) * P_SIZE)
    hydro = hydro.reshape(BX + 2, BY + 2, BZ + 2, P_SIZE, 3)[1:-1, 1:-1, 1:-1]
    hydro = jnp.moveaxis(hydro, -1, 3).reshape(blocks, 3, P_SIZE)

    offsets = block_offsets(27 * P_SIZE + 1, P_SIZE, CX, CY, CZ, R)
    partner_table = jnp.concatenate([records_near[:, 0:3, :], jnp.zeros((blocks, 3, 1), jnp.float32)], axis=2) + offsets[None]
    contact_rows = contacts.reshape(blocks, NC, P_SIZE)
    partner = jax.vmap(lambda table_block, rows_block: jnp.take(table_block, rows_block, axis=1))(partner_table, contact_rows)
    own_records = particles.reshape(blocks, 6, P_SIZE)
    separation = own_records[:, 0:3, None, :] - partner
    valid = (contact_rows < 27 * P_SIZE).astype(jnp.float32)
    square = jnp.sum(separation * separation, axis=1)
    soften = 1.0 + 0.25 * square
    strength = CONTACT_GAIN * valid / (soften * soften)
    contact_force = jnp.sum(separation * strength[:, None], axis=2)
    gravity = jnp.array([0.0, 0.0, GRAVITY_STEP], jnp.float32)
    velocity_new = own_records[:, 3:6] + FORCE_SCALE * hydro + contact_force - gravity[None, :, None]
    position_new = own_records[:, 0:3] + velocity_new * (SPEED_UNIT / R)

    dest_codes = dest_code.reshape(blocks, P_SIZE)
    move_x = dest_codes // 9 - 1
    move_y = (dest_codes // 3) % 3 - 1
    move_z = dest_codes % 3 - 1
    shifted = position_new - jnp.stack([move_x.astype(jnp.float32) * (CX / R), move_y.astype(jnp.float32) * (CY / R),
                                        move_z.astype(jnp.float32) * (CZ / R)], axis=1)
    record = jnp.concatenate([shifted, velocity_new], axis=1)
    home_x = owner_x[:, 0:1]
    home_y = owner_y[:, 0:1]
    home_z = owner_z[:, 0:1]
    target = (((home_x + move_x) * BY + home_y + move_y) * BZ + home_z + move_z) * P_SIZE + dest_slot.reshape(blocks, P_SIZE)
    arrived = jax.ops.segment_sum(jnp.transpose(record, (0, 2, 1)).reshape(-1, 6), target.reshape(-1), num_segments=blocks * P_SIZE)
    arrived = jnp.moveaxis(arrived.reshape(BX, BY, BZ, P_SIZE, 6), -1, 3)
    return populations_next, arrived
```

```python
import functools
import itertools

import jax
import jax.numpy as jnp
from jax import lax
from jax.experimental import pallas as pl
from jax.experimental.pallas import tpu as pltpu
from jax.sharding import PartitionSpec as P

R = 8

LATTICE = [
    (0, 0, 0),
    (1, 0, 0),
    (-1, 0, 0),
    (0, 1, 0),
    (0, -1, 0),
    (0, 0, 1),
    (0, 0, -1),
    (1, 1, 0),
    (-1, -1, 0),
    (1, -1, 0),
    (-1, 1, 0),
    (1, 0, 1),
    (-1, 0, -1),
    (1, 0, -1),
    (-1, 0, 1),
    (0, 1, 1),
    (0, -1, -1),
    (0, 1, -1),
    (0, -1, 1),
]
OPPOSITE = [0, 2, 1, 4, 3, 6, 5, 8, 7, 10, 9, 12, 11, 14, 13, 16, 15, 18, 17]
WEIGHTS = [1.0 / 3.0] + [1.0 / 18.0] * 6 + [1.0 / 36.0] * 12
RELAX_TIME = 0.8
SPEED_UNIT = 0.05
FORCE_SCALE = 0.1
CONTACT_GAIN = 1.0
GRAVITY_STEP = 0.1

MESH = pl.DeviceIdType.MESH
F32 = jnp.float32
BF16 = jnp.bfloat16
I32 = jnp.int32

LEAVING = {
    (axis, sign): [i for i, c in enumerate(LATTICE) if c[axis] == sign]
    for axis in range(3)
    for sign in (1, -1)
}
ORDER = LEAVING[0, 1] + LEAVING[0, -1] + [i for i, c in enumerate(LATTICE) if c[0] == 0]
PLACE = {i: n for n, i in enumerate(ORDER)}
HALOS = [c for c in LATTICE if c != (0, 0, 0)]
HALO_ID = {c: n for n, c in enumerate(HALOS)}
PASS_ORDER = sorted(range(19), key=lambda i: (LATTICE[i][2] != 0, i))
TILES = [c for c in HALOS if c[2] != 0] + [c for c in HALOS if c[2] == 0 and c[0] != 0 and c[1] != 0]
TILE_ID = {c: n for n, c in enumerate(TILES)}
FACES = [(1, 0, 0), (-1, 0, 0), (0, 1, 0), (0, -1, 0), (0, 0, 1), (0, 0, -1)]
LO = 8
GRANT = 16 * 2**20
SUM_UNROLL = 4
EARLY_STEPS = 2
COLLIDE_UNROLL = 2


def side(sign):
    return 0 if sign == 1 else 1


def lane_take(table, index):
    return jnp.take_along_axis(table, index, axis=1, mode="promise_in_bounds")


def nt_dot(left, right):
    return lax.dot_general(left, right, (((1,), (1,)), ((), ())), preferred_element_type=F32)


def split_pair(value):
    high = value.astype(BF16).astype(F32)
    return high, value - high


def kernel(
    sizes,
    shape,
    pops_hbm, frac_hbm, inter_hbm, touch_hbm, part_hbm, cont_hbm, code_hbm, slot_hbm,
    rel, xhalo, yhalo, thalo, moved,
    pv, fv, iv, tv, cv, codev, slotv,
    recs, state, sums, fsend, frecv, ypack, zpack, msend, mrecv,
    in_sem, a_sem, f_sem, h_send, h_recv, m_sem,
):
    X, Y, Z = shape
    slots = recs.shape[3]
    touches = tv.shape[1]
    neighbours = cv.shape[0]
    chunks = X * Y // 8
    halves = Y // 8
    me = tuple(lax.axis_index(a) for a in ("gx", "gy", "gz"))

    own_in = pltpu.make_async_copy(part_hbm, recs.at[13], in_sem.at[0])
    cell_ins = [
        pltpu.make_async_copy(inter_hbm, iv, in_sem.at[1]),
        pltpu.make_async_copy(frac_hbm, fv, in_sem.at[2]),
    ]
    small_ins = [
        pltpu.make_async_copy(src, dst, in_sem.at[3 + n])
        for n, (src, dst) in enumerate(
            [(touch_hbm, tv), (cont_hbm, cv), (code_hbm, codev), (slot_hbm, slotv)]
        )
    ]
    steps = chunks // SUM_UNROLL
    span = SUM_UNROLL * 8

    def pops_in(step):
        rows = pl.ds(pl.multiple_of(step * span, span), span)
        return pltpu.make_async_copy(pops_hbm.at[:, rows], pv.at[:, rows], in_sem.at[7 + step])

    there = {
        (axis, sign): (me[axis] < sizes[axis] - 1) if sign == 1 else (me[axis] > 0)
        for axis in range(3)
        for sign in (1, -1)
    }

    def exists(vector):
        flags = [there[axis, step] for axis, step in enumerate(vector) if step]
        return functools.reduce(lambda p, q: p & q, flags)

    def device(vector):
        return tuple(position + step for position, step in zip(me, vector))

    def each_neighbour(action):
        for o in range(27):
            if o != 13:
                vector = (o // 9 - 1, (o // 3) % 3 - 1, o % 3 - 1)
                pl.when(exists(vector))(functools.partial(action, o, vector))

    own_in.start()
    barrier = pltpu.get_barrier_semaphore()

    def greet(o, vector):
        pl.semaphore_signal(barrier, inc=1, device_id=device(vector), device_id_type=MESH)

    each_neighbour(greet)
    for copy in cell_ins:
        copy.start()
    for step in range(steps):
        pops_in(step).start()
    for copy in small_ins:
        copy.start()

    around = [
        (me[axis] > 0).astype(I32) + (me[axis] < sizes[axis] - 1).astype(I32) for axis in range(3)
    ]
    options = [[0] if size == 1 else [1] if size == 2 else [1, 2] for size in sizes]
    nearby = lambda n: (n[0] + 1) * (n[1] + 1) * (n[2] + 1) - 1
    tiles_near = lambda n: n[2] + n[0] * n[1] + n[0] * n[2] + n[1] * n[2]
    faces_near = lambda n: n[0] + n[1] + n[2]
    count = nearby(around)

    def wait_all(measure, ref, semaphore):
        amount = measure(around)
        for c in sorted({measure(n) for n in itertools.product(*options)}):
            if c:
                part = ref.at[pl.ds(0, c)]
                pl.when(amount == c)(lambda part=part: pltpu.make_async_copy(part, part, semaphore).wait())

    def record_copy(o, vector):
        return pltpu.make_async_remote_copy(
            src_ref=recs.at[13], dst_ref=recs.at[26 - o], send_sem=a_sem.at[0],
            recv_sem=a_sem.at[1], device_id=device(vector), device_id_type=MESH,
        )

    sub8 = lax.broadcasted_iota(I32, (8, Z), 0)
    lane8 = lax.broadcasted_iota(I32, (8, Z), 1)
    high_count = touches // LO
    sub_high = lax.broadcasted_iota(I32, (high_count, Z), 0)

    def gather_pieces(r):
        rows = pl.ds(pl.multiple_of(r * 8, 8), 8)
        f = [pv[i, rows, :] for i in range(19)]
        rho = functools.reduce(lambda a, b: a + b, f)
        momentum = []
        for axis in range(3):
            terms = None
            for i in LEAVING[axis, 1]:
                diff = f[i] - f[OPPOSITE[i]]
                terms = diff if terms is None else terms + diff
            momentum.append(terms)
        index = iv[rows, :]
        eps = fv[rows, :]
        weight = jnp.where(
            index < touches,
            eps * (RELAX_TIME - 0.5) / (1.0 - eps + (RELAX_TIME - 0.5)),
            F32(0.0),
        )
        inverse = 1.0 / rho
        state[0, rows, :] = rho
        for axis in range(3):
            state[1 + axis, rows, :] = momentum[axis] * inverse
        state[4, rows, :] = weight
        wanted = [weight * m for m in momentum] + [weight * rho]
        state[5, rows, :] = wanted[3]
        pairs = [split_pair(w) for w in wanted]
        pieces = [p[0] for p in pairs] + [p[1] for p in pairs]
        high = index // LO if LO & (LO - 1) else lax.shift_right_logical(index, LO.bit_length() - 1)
        low = index - high * LO
        left, right = [], []
        for row in range(8):
            high_row = jnp.broadcast_to(high[row : row + 1], (high_count, Z))
            low_row = jnp.broadcast_to(low[row : row + 1], (8, Z))
            left.append(jnp.where(high_row == sub_high, F32(1.0), F32(0.0)).astype(BF16))
            match = low_row == sub8
            right.append(
                jnp.concatenate(
                    [
                        jnp.where(match, jnp.broadcast_to(p[row : row + 1], (8, Z)), F32(0.0))
                        for p in pieces
                    ],
                    axis=0,
                ).astype(BF16)
            )
        return right, left

    def gather_sums(step, total):
        pops_in(step).wait()
        right, left = [], []
        for n in range(SUM_UNROLL):
            more_right, more_left = gather_pieces(step * SUM_UNROLL + n)
            right += more_right
            left += more_left
        return total + nt_dot(jnp.concatenate(right, axis=1), jnp.concatenate(left, axis=1))

    for copy in cell_ins:
        copy.wait()
    total = jnp.zeros((8 * LO, high_count), F32)
    if EARLY_STEPS:
        total = lax.fori_loop(0, EARLY_STEPS, gather_sums, total)

    own_in.wait()
    pl.semaphore_wait(barrier, count)
    each_neighbour(lambda o, v: record_copy(o, v).start())

    total = lax.fori_loop(EARLY_STEPS, steps, gather_sums, total)
    for copy in small_ins:
        copy.wait()
    sums[...] = jnp.zeros(sums.shape, F32)
    sums[:, 0:high_count] = total[0 : 4 * LO] + total[4 * LO : 8 * LO]

    groups = touches // Z
    parts = []
    for g in range(groups):
        k = lane8 + g * Z
        k_high = lax.shift_right_logical(k, LO.bit_length() - 1)
        k_low = k - k_high * LO
        lines = []
        for q in range(4):
            taken = lane_take(sums[q * LO : (q + 1) * LO, :], k_high)
            lines.append(jnp.sum(jnp.where(k_low == sub8, taken, F32(0.0)), axis=0, keepdims=True))
        quad = jnp.concatenate(lines, axis=0)
        first, second = split_pair(quad)
        parts.append(jnp.concatenate([first, second], axis=0))
    table = jnp.concatenate(parts, axis=1)
    touch_row = tv[...]
    touch_block = lax.shift_right_logical(touch_row, slots.bit_length() - 1)
    touch_slot = touch_row - touch_block * slots
    block8 = jnp.broadcast_to(touch_block, (8, touches))
    spread_left = jnp.concatenate(
        [jnp.where(block8 == o, table, F32(0.0)) for o in range(27)], axis=0
    ).astype(BF16)
    pick = jnp.where(
        jnp.broadcast_to(touch_slot, (slots, touches))
        == lax.broadcasted_iota(I32, (slots, touches), 0),
        F32(1.0),
        F32(0.0),
    ).astype(BF16)
    spread = nt_dot(spread_left, pick)
    for o in range(27):
        piece = spread[o * 8 : (o + 1) * 8]
        fsend[o] = (piece + pltpu.roll(piece, 4, 0))[0:4]

    def force_copy(o, vector):
        return pltpu.make_async_remote_copy(
            src_ref=fsend.at[o], dst_ref=frecv.at[26 - o], send_sem=f_sem.at[0],
            recv_sem=f_sem.at[1], device_id=device(vector), device_id_type=MESH,
        )

    each_neighbour(lambda o, v: force_copy(o, v).start())

    def clear(o):
        recs[o] = jnp.zeros(recs.shape[1:], F32)
        frecv[o] = jnp.zeros(frecv.shape[1:], F32)

    for o in range(27):
        if o != 13:
            vector = (o // 9 - 1, (o // 3) % 3 - 1, o % 3 - 1)
            pl.when(jnp.logical_not(exists(vector)))(functools.partial(clear, o))
    for n, vector in enumerate(FACES):
        back = tuple(-step for step in vector)

        def clear_moved(n=n):
            mrecv[n] = jnp.zeros(mrecv.shape[1:], F32)

        pl.when(jnp.logical_not(exists(back)))(clear_moved)

    code = codev[...]
    wanted_codes = [9 * (v[0] + 1) + 3 * (v[1] + 1) + v[2] + 1 for v in FACES] + [13]
    slot_id = lax.broadcasted_iota(I32, (8, slots), 1).astype(F32) + 1.0
    code_of = jnp.full((8, slots), 27, I32)
    row_id = lax.broadcasted_iota(I32, (8, slots), 0)
    for n, c in enumerate(wanted_codes):
        code_of = jnp.where(row_id == n, c, code_of)
    route = jnp.where(jnp.broadcast_to(code, (8, slots)) == code_of, slot_id, F32(0.0)).astype(BF16)
    place = jnp.where(
        jnp.broadcast_to(slotv[...], (slots, slots)) == lax.broadcasted_iota(I32, (slots, slots), 0),
        F32(1.0),
        F32(0.0),
    ).astype(BF16)
    taken_from = nt_dot(route, place).astype(I32)

    def dot(c, vec):
        value = None
        for axis in range(3):
            if c[axis]:
                term = vec[axis] if c[axis] == 1 else -vec[axis]
                value = term if value is None else value + term
        return value

    def collide_fluid(r):
        rows = pl.ds(pl.multiple_of(r * 8, 8), 8)
        rho = state[0, rows, :]
        u = [state[1 + d, rows, :] for d in range(3)]
        weight = state[4, rows, :]
        keep = (1.0 - weight) * (1.0 / RELAX_TIME)
        rest_u = 1.0 - 1.5 * (u[0] * u[0] + u[1] * u[1] + u[2] * u[2])
        scaled = {w: w * rho for w in sorted(set(WEIGHTS))}
        f0 = pv[0, rows, :]
        eq_u = scaled[WEIGHTS[0]] * rest_u
        rel[PLACE[0], rows, :] = f0 - keep * (f0 - eq_u) - weight * eq_u
        for i in range(1, 19, 2):
            j = OPPOSITE[i]
            share = scaled[WEIGHTS[i]]
            pu = dot(LATTICE[i], u)
            even = share * (rest_u + 4.5 * pu * pu)
            odd = share * (3.0 * pu)
            fi, fj = pv[i, rows, :], pv[j, rows, :]
            ui, uj = even + odd, even - odd
            diff = fj - fi
            rel[PLACE[i], rows, :] = fi - keep * (fi - ui) + weight * (diff - uj)
            rel[PLACE[j], rows, :] = fj - keep * (fj - uj) - weight * (diff + ui)

    def collide_some(step, carry):
        for n in range(COLLIDE_UNROLL):
            collide_fluid(step * COLLIDE_UNROLL + n)
        return carry

    lax.fori_loop(0, chunks // COLLIDE_UNROLL, collide_some, 0)

    edges = {(axis, sign): n for n, (axis, sign) in enumerate([(1, 1), (1, -1), (2, 1), (2, -1)])}
    edge_index, edge_share, line_of = {}, {}, {}
    for sign in (1, -1):
        line = pl.ds(Y - 1 if sign == 1 else 0, X, stride=Y)
        for entry, i in enumerate(LEAVING[1, sign]):
            ypack[side(sign), entry] = rel[PLACE[i], line, :]
        line_of[sign] = line

    def pack_columns(read, entries, edge, start):
        packed = start
        for entry in range(entries):
            for r in range(chunks):
                column = entry * chunks + r
                turned = read(entry, pl.ds(r * 8, 8))
                if (column - edge) % Z:
                    turned = pltpu.roll(turned, (column - edge) % Z, 1)
                packed = jnp.where(lane8 == column, turned, packed)
        return packed

    repeat = lax.rem(lane8, chunks)
    for sign in (1, -1):
        edge = Z - 1 if sign == 1 else 0
        leaving = LEAVING[2, sign]
        zpack[side(sign)] = pack_columns(
            lambda entry, rows: rel[PLACE[leaving[entry]], rows, :], 5, edge, jnp.zeros((8, Z), F32)
        )
        share = pack_columns(lambda entry, rows: state[5, rows, :], 1, edge, jnp.zeros((8, Z), F32))
        index = pack_columns(
            lambda entry, rows: iv[rows, :], 1, edge, jnp.full((8, Z), touches, I32)
        )
        edge_share[sign] = lane_take(share, repeat)
        edge_index[sign] = lane_take(index, repeat)

    wait_all(nearby, recs, a_sem.at[1])

    index_rows = [touch_row[:, g * Z : (g + 1) * Z] for g in range(groups)]
    touch8 = jnp.concatenate(
        index_rows + [jnp.full((8 - groups, Z), 27 * slots, I32)], axis=0
    )

    def fetch(first_row, index):
        found = [jnp.zeros((8, Z), F32)] * 3
        block = lax.shift_right_logical(index, slots.bit_length() - 1)
        local = index - block * slots
        for o in range(27):
            hit = block == o
            for d in range(3):
                row = jnp.broadcast_to(recs[o, first_row + d], (8, Z))
                found[d] = jnp.where(hit, lane_take(row, local), found[d])
        return found

    touch_velocity = [SPEED_UNIT * v for v in fetch(3, touch8)]
    tables = [
        [jnp.broadcast_to(touch_velocity[d][g : g + 1], (8, Z)) for g in range(groups)]
        for d in range(3)
    ]

    def solid_velocity(index):
        group = lax.shift_right_logical(index, Z.bit_length() - 1)
        local = index - group * Z
        v = []
        for d in range(3):
            value = jnp.zeros((8, Z), F32)
            for g in range(groups):
                value = jnp.where(group == g, lane_take(tables[d][g], local), value)
            v.append(value)
        return v, 1.0 - 1.5 * (v[0] * v[0] + v[1] * v[1] + v[2] * v[2])

    def halo_copy(vector):
        m = 2 if vector[2] != 0 or (vector[0] != 0 and vector[1] != 0) else 0 if vector[0] != 0 else 1
        if vector[2] != 0:
            src, dst = zpack.at[side(vector[2])], thalo.at[TILE_ID[vector]]
        elif vector[0] != 0 and vector[1] != 0:
            entry = LEAVING[1, vector[1]].index(LATTICE.index(vector))
            src, dst = ypack.at[side(vector[1]), entry], thalo.at[TILE_ID[vector]]
        elif vector[0] != 0:
            start = 5 * side(vector[0])
            row = (X - 1) * Y if vector[0] == 1 else 0
            src = rel.at[pl.ds(start, 5), pl.ds(row, Y), :]
            dst = xhalo.at[side(vector[0])]
        else:
            src, dst = ypack.at[side(vector[1])], yhalo.at[side(vector[1])]
        return pltpu.make_async_remote_copy(
            src_ref=src, dst_ref=dst, send_sem=h_send.at[m], recv_sem=h_recv.at[m],
            device_id=device(vector), device_id_type=MESH,
        )

    def when_there(vector, action):
        pl.when(exists(vector))(action)

    entry8 = lane8 // chunks
    for sign in (1, -1):
        v, rest = solid_velocity(edge_index[sign])
        along = v[2] if sign == 1 else -v[2]
        base = jnp.zeros((8, Z), F32)
        for entry, i in enumerate(LEAVING[2, sign]):
            here = entry8 == entry
            base = jnp.where(here, F32(WEIGHTS[i]), base)
            for d in range(2):
                c = LATTICE[i][d]
                if c:
                    along = jnp.where(here, along + v[d] if c == 1 else along - v[d], along)
        zpack[side(sign)] = zpack[side(sign)] + edge_share[sign] * base * (
            rest + (4.5 * along + 3.0) * along
        )
    for sign in (1, -1):
        v, rest = solid_velocity(iv[line_of[sign], :])
        share = state[5, line_of[sign], :]
        for entry, i in enumerate(LEAVING[1, sign]):
            along = dot(LATTICE[i], v)
            ypack[side(sign), entry] = ypack[side(sign), entry] + share * F32(WEIGHTS[i]) * (
                rest + (4.5 * along + 3.0) * along
            )
    for vector in HALOS:
        if vector[2] != 0 or vector[1] != 0:
            when_there(vector, lambda vector=vector: halo_copy(vector).start())

    def collide_solid(r):
        rows = pl.ds(pl.multiple_of(r * 8, 8), 8)
        v, rest = solid_velocity(iv[rows, :])
        share = state[5, rows, :]
        scaled = {w: w * share for w in sorted(set(WEIGHTS))}
        rel[PLACE[0], rows, :] = rel[PLACE[0], rows, :] + scaled[WEIGHTS[0]] * rest
        for i in range(1, 19, 2):
            j = OPPOSITE[i]
            ps = dot(LATTICE[i], v)
            even = scaled[WEIGHTS[i]] * (rest + 4.5 * ps * ps)
            odd = scaled[WEIGHTS[i]] * (3.0 * ps)
            rel[PLACE[i], rows, :] = rel[PLACE[i], rows, :] + (even + odd)
            rel[PLACE[j], rows, :] = rel[PLACE[j], rows, :] + (even - odd)

    for x in sorted({0, X - 1}):
        for h in range(halves):
            collide_solid(x * halves + h)
    for vector in HALOS:
        if vector[1] == 0 and vector[2] == 0:
            when_there(vector, lambda vector=vector: halo_copy(vector).start())

    own = [recs[13, d] for d in range(6)]
    contact = [jnp.zeros((1, slots), F32) for _ in range(3)]
    spans = (X / R, Y / R, Z / R)
    for start in range(0, neighbours, 8):
        stop = min(start + 8, neighbours)
        lines = [cv[n] for n in range(start, stop)]
        if stop - start < 8:
            lines.append(jnp.full((8 - stop + start, slots), 27 * slots, I32))
        entries = jnp.concatenate(lines, axis=0)
        found = fetch(0, entries)
        block = lax.shift_right_logical(entries, slots.bit_length() - 1)
        nine = jnp.zeros(block.shape, I32)
        for step in (9, 18, 27):
            nine = nine + (block >= step).astype(I32)
        inner = block - 9 * nine
        three = (inner >= 3).astype(I32) + (inner >= 6).astype(I32)
        moves = (nine - 1, three - 1, inner - 3 * three - 1)
        apart = [
            jnp.broadcast_to(own[d], (8, slots)) - (found[d] + moves[d].astype(F32) * spans[d])
            for d in range(3)
        ]
        soften = 1.0 + 0.25 * (apart[0] * apart[0] + apart[1] * apart[1] + apart[2] * apart[2])
        strength = CONTACT_GAIN * (entries < 27 * slots).astype(F32) / (soften * soften)
        for d in range(3):
            contact[d] = contact[d] + jnp.sum(apart[d] * strength, axis=0, keepdims=True)

    wait_all(nearby, frecv, f_sem.at[1])
    force = fsend[13]
    for o in range(27):
        if o != 13:
            force = force + frecv[o]
    gravity = (0.0, 0.0, GRAVITY_STEP)
    velocity_new, position_new = [], []
    for d in range(3):
        speed = own[3 + d]
        hydro = force[d : d + 1] - force[3:4] * (SPEED_UNIT * speed)
        velocity = speed + FORCE_SCALE * hydro + contact[d] - gravity[d]
        velocity_new.append(velocity)
        position_new.append(own[d] + velocity * (SPEED_UNIT / R))
    record = jnp.concatenate(position_new + velocity_new + [jnp.zeros((2, slots), F32)], axis=0)

    def routed(n, vector):
        origin = jnp.broadcast_to(taken_from[n : n + 1], (8, slots))
        moved = lane_take(record, jnp.where(origin > 0, origin - 1, 0))
        shift = jnp.zeros((8, slots), F32)
        for d in range(3):
            if vector[d]:
                shift = jnp.where(row_id == d, F32(vector[d] * spans[d]), shift)
        return jnp.where(origin > 0, moved - shift, F32(0.0))

    def move_copy(n):
        return pltpu.make_async_remote_copy(
            src_ref=msend.at[n], dst_ref=mrecv.at[n], send_sem=m_sem.at[0],
            recv_sem=m_sem.at[1], device_id=device(FACES[n]), device_id_type=MESH,
        )

    for n, vector in enumerate(FACES):
        msend[n] = routed(n, vector)
        when_there(vector, lambda n=n: move_copy(n).start())
    stay = routed(6, (0, 0, 0))

    def collide_rest(step, carry):
        for n in range(COLLIDE_UNROLL):
            collide_solid(halves + step * COLLIDE_UNROLL + n)
        return carry

    lax.fori_loop(0, (X - 2) * halves // COLLIDE_UNROLL, collide_rest, 0)

    wait_all(nearby, recs, a_sem.at[0])
    wait_all(nearby, fsend, f_sem.at[0])
    wait_all(lambda n: n[0], xhalo, h_send.at[0])
    wait_all(lambda n: n[1], yhalo, h_send.at[1])
    wait_all(tiles_near, thalo, h_send.at[2])
    wait_all(faces_near, msend, m_sem.at[0])
    wait_all(faces_near, mrecv, m_sem.at[1])
    for n in range(len(FACES)):
        stay = stay + mrecv[n]
    for d in range(6):
        moved[d] = stay[d : d + 1]
    wait_all(lambda n: n[0], xhalo, h_recv.at[0])
    wait_all(lambda n: n[1], yhalo, h_recv.at[1])
    wait_all(tiles_near, thalo, h_recv.at[2])


def pass_kernel(sizes, shape, rel, xhalo, yhalo, thalo, moved, out_hbm, part_out, pv, out_sem):
    X, Y, Z = shape
    chunks = X * Y // 8
    halves = Y // 8
    me = tuple(lax.axis_index(a) for a in ("gx", "gy", "gz"))
    part_copy = pltpu.make_async_copy(moved, part_out, out_sem.at[1])
    part_copy.start()
    suby = lax.broadcasted_iota(I32, (Y, Z), 0)
    laney = lax.broadcasted_iota(I32, (Y, Z), 1)
    open_back = {
        (axis, sign): (me[axis] > 0) if sign == 1 else (me[axis] < sizes[axis] - 1)
        for axis in range(3)
        for sign in (1, -1)
    }
    target = {1: 0, -1: Z - 1}
    row_edge = {1: 0, -1: Y - 1}

    def edge_mask(c):
        mask = None
        if c[1]:
            blocked = jnp.broadcast_to(jnp.where(open_back[1, c[1]], -1, row_edge[c[1]]), (Y, Z))
            mask = suby != blocked
        if c[2]:
            blocked = jnp.broadcast_to(jnp.where(open_back[2, c[2]], -1, target[c[2]]), (Y, Z))
            other = laney != blocked
            mask = other if mask is None else mask & other
        return mask

    for i in PASS_ORDER:
        c = LATTICE[i]
        j = OPPOSITE[i]
        mask = edge_mask(c)
        for x in range(X):
            from_x = x - c[0]
            inside_x = 0 <= from_x < X
            wrapped = from_x % X
            if inside_x:
                slab = rel[PLACE[i], from_x * Y : (from_x + 1) * Y, :]
            else:
                slab = xhalo[side(c[0]), LEAVING[0, c[0]].index(i)]
            turn = 1 if c[2] == 1 else Z - 1
            if c[2]:
                entry = LEAVING[2, c[2]].index(i)
                tile = thalo[TILE_ID[(0, 0, c[2])]] if inside_x else thalo[TILE_ID[(c[0], 0, c[2])]]
                columns = []
                for h in range(halves):
                    column = entry * chunks + wrapped * halves + h
                    amount = (target[c[2]] - column) % Z
                    columns.append(pltpu.roll(tile, amount, 1) if amount else tile)
                edge_columns = jnp.concatenate(columns, axis=0)
                slab = jnp.where(laney == target[c[2]], edge_columns, pltpu.roll(slab, turn, 1))
            if c[1]:
                entry = LEAVING[1, c[1]].index(i)
                if inside_x:
                    line = yhalo[side(c[1]), entry, from_x : from_x + 1, :]
                else:
                    line = thalo[TILE_ID[(c[0], c[1], 0)], wrapped : wrapped + 1, :]
                if c[2]:
                    entry = LEAVING[2, c[2]].index(i)
                    last = (Y - 1) if c[1] == 1 else 0
                    column = entry * chunks + from_x * halves + last // 8
                    amount = (target[c[2]] - column) % Z
                    tile = thalo[TILE_ID[c]]
                    tile = pltpu.roll(tile, amount, 1) if amount else tile
                    corner = tile[last % 8 : last % 8 + 1]
                    tile = yhalo[side(c[1]), LEAVING[1, c[1]].index(i)]
                    line = pltpu.roll(tile, turn, 1)[from_x : from_x + 1]
                    line = jnp.where(laney[0:1] == target[c[2]], corner, line)
                slab = pltpu.roll(slab, 1 if c[1] == 1 else Y - 1, 0)
                slab = jnp.where(suby == row_edge[c[1]], jnp.broadcast_to(line, (Y, Z)), slab)
            mirror = rel[PLACE[j], x * Y : (x + 1) * Y, :] if c != (0, 0, 0) else None
            if mask is not None:
                slab = jnp.where(mask, slab, mirror)
            if not inside_x:
                closed = jnp.broadcast_to(open_back[0, c[0]].astype(I32), (Y, Z))
                slab = jnp.where(closed > 0, slab, mirror)
            pv[i, x * Y : (x + 1) * Y, :] = slab
        pltpu.make_async_copy(pv.at[i], out_hbm.at[i], out_sem.at[0]).start()

    part_copy.wait()
    pltpu.make_async_copy(pv, out_hbm, out_sem.at[0]).wait()


def body(sizes, populations, solid_fraction, intersection, touch, particles, contacts, dest_code, dest_slot):
    count, X, Y, Z = populations.shape
    slots = particles.shape[4]
    touches = touch.shape[3]
    neighbours = contacts.shape[3]
    any_space = pl.BlockSpec(memory_space=pl.ANY)
    dma = pltpu.SemaphoreType.DMA
    vmem = pl.BlockSpec(memory_space=pltpu.VMEM)
    values = (
        populations.reshape(count, X * Y, Z),
        solid_fraction.reshape(X * Y, Z),
        intersection.reshape(X * Y, Z),
        touch.reshape(1, touches),
        particles.reshape(6, 1, slots),
        contacts.reshape(neighbours, 1, slots),
        dest_code.reshape(1, slots),
        dest_slot.reshape(1, slots),
    )
    handed = pl.pallas_call(
        functools.partial(kernel, sizes, (X, Y, Z)),
        out_shape=(
            pltpu.VMEM((count, X * Y, Z), F32),
            pltpu.VMEM((2, 5, Y, Z), F32),
            pltpu.VMEM((2, 5, X, Z), F32),
            pltpu.VMEM((len(TILES), 8, Z), F32),
            pltpu.VMEM((6, 1, slots), F32),
        ),
        in_specs=[pl.BlockSpec(memory_space=pltpu.HBM)] * 8,
        out_specs=(vmem,) * 5,
        scratch_shapes=[
            pltpu.VMEM((count, X * Y, Z), F32),
            pltpu.VMEM((X * Y, Z), F32),
            pltpu.VMEM((X * Y, Z), I32),
            pltpu.VMEM((1, touches), I32),
            pltpu.VMEM((neighbours, 1, slots), I32),
            pltpu.VMEM((1, slots), I32),
            pltpu.VMEM((1, slots), I32),
            pltpu.VMEM((27, 6, 1, slots), F32),
            pltpu.VMEM((6, X * Y, Z), F32),
            pltpu.VMEM((4 * LO, Z), F32),
            pltpu.VMEM((27, 4, slots), F32),
            pltpu.VMEM((27, 4, slots), F32),
            pltpu.VMEM((2, 5, X, Z), F32),
            pltpu.VMEM((2, 8, Z), F32),
            pltpu.VMEM((len(FACES), 8, slots), F32),
            pltpu.VMEM((len(FACES), 8, slots), F32),
            dma((7 + X * Y // (8 * SUM_UNROLL),)),
            dma((2,)),
            dma((2,)),
            dma((3,)),
            dma((3,)),
            dma((2,)),
        ],
        compiler_params=pltpu.CompilerParams(
            collective_id=0, has_side_effects=True, vmem_limit_bytes=GRANT
        ),
    )(*[pltpu.with_memory_space_constraint(value, pltpu.HBM) for value in values])
    out, moved = pl.pallas_call(
        functools.partial(pass_kernel, sizes, (X, Y, Z)),
        out_shape=(
            jax.ShapeDtypeStruct((count, X * Y, Z), F32),
            jax.ShapeDtypeStruct((6, 1, slots), F32),
        ),
        in_specs=[vmem] * 5,
        out_specs=(any_space, any_space),
        scratch_shapes=[pltpu.VMEM((count, X * Y, Z), F32), dma((2,))],
        compiler_params=pltpu.CompilerParams(vmem_limit_bytes=GRANT),
    )(*[pltpu.with_memory_space_constraint(value, pltpu.VMEM) for value in handed])
    return (out.reshape(count, X, Y, Z), moved.reshape(1, 1, 1, 6, slots))


def solution(mesh):
    placed = (
        P(None, "gx", "gy", "gz"),
        P("gx", "gy", "gz"),
        P("gx", "gy", "gz"),
        P("gx", "gy", "gz", None),
        P("gx", "gy", "gz", None, None),
        P("gx", "gy", "gz", None, None),
        P("gx", "gy", "gz", None),
        P("gx", "gy", "gz", None),
    )
    sizes = tuple(mesh.shape[axis] for axis in ("gx", "gy", "gz"))
    return jax.shard_map(
        functools.partial(body, sizes),
        mesh=mesh,
        in_specs=placed,
        out_specs=(P(None, "gx", "gy", "gz"), P("gx", "gy", "gz", None, None)),
        check_vma=False,
    )
```

```python
import functools
import itertools

import jax
import jax.numpy as jnp
from jax import lax
from jax.experimental import pallas as pl
from jax.experimental.pallas import tpu as pltpu
from jax.sharding import PartitionSpec as P

R = 8

LATTICE = [
    (0, 0, 0),
    (1, 0, 0),
    (-1, 0, 0),
    (0, 1, 0),
    (0, -1, 0),
    (0, 0, 1),
    (0, 0, -1),
    (1, 1, 0),
    (-1, -1, 0),
    (1, -1, 0),
    (-1, 1, 0),
    (1, 0, 1),
    (-1, 0, -1),
    (1, 0, -1),
    (-1, 0, 1),
    (0, 1, 1),
    (0, -1, -1),
    (0, 1, -1),
    (0, -1, 1),
]
OPPOSITE = [0, 2, 1, 4, 3, 6, 5, 8, 7, 10, 9, 12, 11, 14, 13, 16, 15, 18, 17]
WEIGHTS = [1.0 / 3.0] + [1.0 / 18.0] * 6 + [1.0 / 36.0] * 12
RELAX_TIME = 0.8
SPEED_UNIT = 0.05
FORCE_SCALE = 0.1
CONTACT_GAIN = 1.0
GRAVITY_STEP = 0.1

MESH = pl.DeviceIdType.MESH
F32 = jnp.float32
BF16 = jnp.bfloat16
I32 = jnp.int32

LEAVING = {
    (axis, sign): [i for i, c in enumerate(LATTICE) if c[axis] == sign]
    for axis in range(3)
    for sign in (1, -1)
}
ORDER = LEAVING[0, 1] + LEAVING[0, -1] + [i for i, c in enumerate(LATTICE) if c[0] == 0]
PLACE = {i: n for n, i in enumerate(ORDER)}
HALOS = [c for c in LATTICE if c != (0, 0, 0)]
HALO_ID = {c: n for n, c in enumerate(HALOS)}
PASS_ORDER = sorted(range(19), key=lambda i: (LATTICE[i][2] != 0, i))
TILES = [c for c in HALOS if c[2] != 0] + [c for c in HALOS if c[2] == 0 and c[0] != 0 and c[1] != 0]
TILE_ID = {c: n for n, c in enumerate(TILES)}
FACES = [(1, 0, 0), (-1, 0, 0), (0, 1, 0), (0, -1, 0), (0, 0, 1), (0, 0, -1)]
LO = 8
GRANT = 16 * 2**20
SUM_UNROLL = 8
EARLY_STEPS = 1
COLLIDE_UNROLL = 2
SOLID_UNROLL = 6
BEYOND = (1, 1, 1)
BEFORE = (-1, -1, -1)


def block_id(vector):
    return 9 * (vector[0] + 1) + 3 * (vector[1] + 1) + vector[2] + 1


def side(sign):
    return 0 if sign == 1 else 1


def lane_take(table, index):
    return jnp.take_along_axis(table, index, axis=1, mode="promise_in_bounds")


def nt_dot(left, right):
    return lax.dot_general(left, right, (((1,), (1,)), ((), ())), preferred_element_type=F32)


def split_pair(value):
    high = value.astype(BF16).astype(F32)
    return high, value - high


def kernel(
    sizes,
    shape,
    pops_hbm, frac_hbm, inter_hbm, touch_hbm, part_hbm, cont_hbm, code_hbm, slot_hbm,
    rel, xhalo, yhalo, thalo, moved,
    pv, fv, iv, tv, cv, codev, slotv,
    recs, state, sums, fsend, frecv, ypack, zpack, msend, mrecv,
    picked, ruler, in_sem, sent, recs_in, forces_in, edges_in, ready,
):
    X, Y, Z = shape
    slots = recs.shape[3]
    touches = tv.shape[1]
    neighbours = cv.shape[0]
    chunks = X * Y // 8
    halves = Y // 8
    me = tuple(lax.axis_index(a) for a in ("gx", "gy", "gz"))

    cell_ins = [
        pltpu.make_async_copy(inter_hbm, iv, in_sem.at[1]),
        pltpu.make_async_copy(frac_hbm, fv, in_sem.at[1]),
    ]
    small_ins = [
        pltpu.make_async_copy(src, dst, in_sem.at[0])
        for src, dst in [
            (part_hbm, recs.at[13]), (touch_hbm, tv), (cont_hbm, cv), (code_hbm, codev),
            (slot_hbm, slotv),
        ]
    ]
    small_rows = (touches + (neighbours + 8) * slots) // Z
    cells_done = pltpu.make_async_copy(pops_hbm.at[0:2], pv.at[0:2], in_sem.at[1])
    small_done = pltpu.make_async_copy(
        pops_hbm.at[0, 0:small_rows], pv.at[0, 0:small_rows], in_sem.at[0]
    )
    steps = chunks // SUM_UNROLL
    span = SUM_UNROLL * 8

    def pops_in(step):
        rows = pl.ds(pl.multiple_of(step * span, span), span)
        return pltpu.make_async_copy(pops_hbm.at[:, rows], pv.at[:, rows], in_sem.at[2 + step])

    there = {
        (axis, sign): (me[axis] < sizes[axis] - 1) if sign == 1 else (me[axis] > 0)
        for axis in range(3)
        for sign in (1, -1)
    }

    def exists(vector):
        flags = [there[axis, step] for axis, step in enumerate(vector) if step]
        return functools.reduce(lambda p, q: p & q, flags)

    def device(vector):
        return tuple(position + step for position, step in zip(me, vector))

    def steps_along(axis):
        if sizes[axis] == 1:
            return [((0,), None)]
        if sizes[axis] == 2:
            return [((0, 1 - 2 * me[axis]), None)]
        return [((-1,), there[axis, -1]), ((0,), None), ((1,), there[axis, 1])]

    def far(vector):
        return sum(1 for step in vector if not (isinstance(step, int) and step == 0))

    def each_neighbour(action, skip=(2, 2, 2), allow={}, levels=(-1, 0, 1)):
        groups = []
        for choice in itertools.product(*[steps_along(axis) for axis in range(3)]):
            level = choice[2][0][0]
            if sizes[2] > 2 and level not in levels:
                continue
            flags = [flag for _, flag in choice if flag is not None]
            if level in allow:
                flags.append(allow[level])
            vectors = list(itertools.product(*[values for values, _ in choice]))
            groups.append((flags, sorted([v for v in vectors if far(v)], key=far, reverse=True)))

        def act(vectors):
            for vector in vectors:
                do = functools.partial(action, block_id(vector), vector)
                pairs = list(zip(range(3), vector, skip))
                fixed = [p for p in pairs if isinstance(p[1], int)]
                moving = [p for p in pairs if not isinstance(p[1], int)]
                if any(step != other for _, step, other in fixed) or 2 in skip:
                    do()
                elif moving and all(other for _, _, other in moving):
                    apart = [jnp.logical_not(there[axis, other]) for axis, _, other in moving]
                    pl.when(functools.reduce(lambda p, q: p | q, apart))(do)
                elif moving:
                    do()

        for flags, vectors in sorted(groups, key=lambda g: max(map(far, g[1]), default=0), reverse=True):
            run = functools.partial(act, vectors)
            if flags:
                pl.when(functools.reduce(lambda p, q: p & q, flags))(run)
            else:
                run()

    windows = [
        [0] if size == 1 else [0 - at, 1 - at] if size == 2 else [-1, 0, 1]
        for size, at in zip(sizes, me)
    ]
    blocks = [block_id((x, y, z)) for x in windows[0] for y in windows[1] for z in windows[2]]

    barrier = pltpu.get_barrier_semaphore()

    half = sizes[2] // 2
    split = sizes[2] > 2
    alone_up = there[2, 1] & (me[2] >= half)
    alone_down = me[2] > half
    not_up = {1: jnp.logical_not(alone_up)} if split else {}
    not_down = {-1: jnp.logical_not(alone_down)} if split else {}

    def greet(o, vector):
        pl.semaphore_signal(barrier, inc=1, device_id=device(vector), device_id_type=MESH)

    for copy in small_ins:
        copy.start()
    for copy in cell_ins:
        copy.start()
    for step in range(steps):
        pops_in(step).start()
    each_neighbour(greet, BEFORE, not_down)

    around = [
        (me[axis] > 0).astype(I32) + (me[axis] < sizes[axis] - 1).astype(I32) for axis in range(3)
    ]
    options = [[0] if size == 1 else [1] if size == 2 else [1, 2] for size in sizes]
    nearby = lambda n: (n[0] + 1) * (n[1] + 1) * (n[2] + 1) - 1
    record_rows = lambda n: 6 * nearby(n)
    force_rows = lambda n: 4 * nearby(n)

    def edge_rows(n):
        x, y, z = n
        tiles = 8 * (z + x * z + x + y + z) + x * y + y * z
        return 5 * (Y * x + X * y) + tiles

    sent_rows = lambda n: record_rows(n) + force_rows(n) + edge_rows(n)

    plane = (around[0] + 1) * (around[1] + 1)
    waiting = exists(BEYOND).astype(I32)
    if split:
        waiting = jnp.where(alone_up, plane, waiting)
    count = nearby(around) - waiting

    def wait_rows(measure, semaphore):
        amount = measure(around)
        for rows in sorted({measure(n) for n in itertools.product(*options)}):
            if rows:
                part = ruler.at[0:rows]
                copy = pltpu.make_async_copy(part, part, semaphore.at[0])
                pl.when(amount == rows)(copy.wait)

    def record_copy(o, vector):
        return pltpu.make_async_remote_copy(
            src_ref=recs.at[13], dst_ref=recs.at[26 - o], send_sem=sent.at[0],
            recv_sem=recs_in.at[0], device_id=device(vector), device_id_type=MESH,
        )

    sub8 = lax.broadcasted_iota(I32, (8, Z), 0)
    lane8 = lax.broadcasted_iota(I32, (8, Z), 1)
    high_count = touches // LO
    sub_high = lax.broadcasted_iota(I32, (high_count, Z), 0)

    def gather_pieces(r):
        rows = pl.ds(pl.multiple_of(r * 8, 8), 8)
        f = [pv[i, rows, :] for i in range(19)]
        rho = functools.reduce(lambda a, b: a + b, f)
        momentum = []
        for axis in range(3):
            terms = None
            for i in LEAVING[axis, 1]:
                diff = f[i] - f[OPPOSITE[i]]
                terms = diff if terms is None else terms + diff
            momentum.append(terms)
        index = iv[rows, :]
        eps = fv[rows, :]
        weight = jnp.where(
            index < touches,
            eps * (RELAX_TIME - 0.5) / (1.0 - eps + (RELAX_TIME - 0.5)),
            F32(0.0),
        )
        inverse = 1.0 / rho
        state[0, rows, :] = rho
        for axis in range(3):
            state[1 + axis, rows, :] = momentum[axis] * inverse
        state[4, rows, :] = weight
        wanted = [weight * m for m in momentum] + [weight * rho]
        state[5, rows, :] = wanted[3]
        pairs = [split_pair(w) for w in wanted]
        pieces = [p[0] for p in pairs] + [p[1] for p in pairs]
        high = index // LO if LO & (LO - 1) else lax.shift_right_logical(index, LO.bit_length() - 1)
        low = index - high * LO
        return pieces, high, low

    def gather_pairs(pieces, high, low):
        left, right = [], []
        for row in range(8):
            high_row = jnp.broadcast_to(high[row : row + 1], (high_count, Z))
            match = jnp.broadcast_to(low[row : row + 1], (8, Z)) == sub8
            left.append(jnp.where(high_row == sub_high, F32(1.0), F32(0.0)).astype(BF16))
            right.append(
                jnp.concatenate(
                    [
                        jnp.where(match, jnp.broadcast_to(pieces[p][row : row + 1], (8, Z)), F32(0.0))
                        for p in range(8)
                    ],
                    axis=0,
                ).astype(BF16)
            )
        return right, left

    def gather_sums(step, total):
        pops_in(step).wait()
        right, left = [], []
        for n in range(SUM_UNROLL):
            more_right, more_left = gather_pairs(*gather_pieces(step * SUM_UNROLL + n))
            right += more_right
            left += more_left
        return total + nt_dot(jnp.concatenate(left, axis=1), jnp.concatenate(right, axis=1))

    groups = touches // Z

    def spread_sums(total):
        sums[:, 0 : 8 * LO] = total
        both = sums[...]
        both = both + pltpu.roll(both, Z - 4 * LO, 1)
        lane_high = lax.shift_right_logical(lane8, LO.bit_length() - 1)
        lane_low = lane8 - lane_high * LO
        parts = []
        for g in range(groups):
            lines = []
            for q in range(4):
                line = jnp.zeros((8, Z), F32)
                for part in range(Z // (8 * LO)):
                    first_row = g * (Z // LO) + part * 8
                    taken = lane_take(both[first_row : first_row + 8], q * LO + lane_low)
                    line = line + jnp.where(sub8 + part * 8 == lane_high, taken, F32(0.0))
                lines.append(jnp.sum(line, axis=0, keepdims=True))
            quad = jnp.concatenate(lines, axis=0)
            first, second = split_pair(quad)
            parts.append(jnp.concatenate([first, second], axis=0))
        table = jnp.concatenate(parts, axis=1)
        block8 = jnp.broadcast_to(touch_block, (8, touches))
        spread_left = jnp.concatenate(
            [jnp.where(block8 == o, table, F32(0.0)) for o in blocks], axis=0
        ).astype(BF16)
        spread = nt_dot(spread_left, picked[...])
        for n, o in enumerate(blocks):
            piece = spread[n * 8 : (n + 1) * 8]
            fsend[o] = (piece + pltpu.roll(piece, 4, 0))[0:4]

    middle = (lax.rem(me[0], 2) == 1) & there[0, 1]
    idle = (there[1, 1] & there[2, 1]) | (middle & (there[1, 1] | there[2, 1]))
    if split:
        idle = idle & ((me[2] < half) | middle)
    first_steps = jnp.where(idle, steps, EARLY_STEPS)
    if split:
        late = (me[2] >= half) & jnp.logical_not(idle)
        first_steps = jnp.where(late & jnp.logical_not(there[1, 1]), 0, first_steps)
    sums[...] = jnp.zeros(sums.shape, F32)
    frecv[13] = jnp.zeros(frecv.shape[1:], F32)

    def clear(ids):
        for o in ids:
            recs[o] = jnp.zeros(recs.shape[1:], F32)
            frecv[o] = jnp.zeros(frecv.shape[1:], F32)

    for choice in itertools.product(*[steps_along(axis) for axis in range(3)]):
        flags = [flag for _, flag in choice if flag is not None]
        if flags:
            ids = [block_id(vector) for vector in itertools.product(*[values for values, _ in choice])]
            present = functools.reduce(lambda p, q: p & q, flags)
            pl.when(jnp.logical_not(present))(functools.partial(clear, ids))
    for n, vector in enumerate(FACES):
        back = tuple(-step for step in vector)

        def clear_moved(n=n):
            mrecv[n] = jnp.zeros(mrecv.shape[1:], F32)

        pl.when(jnp.logical_not(exists(back)))(clear_moved)

    small_done.wait()
    touch_row = tv[...]
    touch_block = lax.shift_right_logical(touch_row, slots.bit_length() - 1)
    touch_slot = touch_row - touch_block * slots
    picked[...] = jnp.where(
        jnp.broadcast_to(touch_slot, (slots, touches))
        == lax.broadcasted_iota(I32, (slots, touches), 0),
        F32(1.0),
        F32(0.0),
    ).astype(BF16)

    code = codev[...]
    wanted_codes = [9 * (v[0] + 1) + 3 * (v[1] + 1) + v[2] + 1 for v in FACES] + [13]
    slot_id = lax.broadcasted_iota(I32, (8, slots), 1).astype(F32) + 1.0
    code_of = jnp.full((8, slots), 27, I32)
    row_id = lax.broadcasted_iota(I32, (8, slots), 0)
    for n, c in enumerate(wanted_codes):
        code_of = jnp.where(row_id == n, c, code_of)
    route = jnp.where(jnp.broadcast_to(code, (8, slots)) == code_of, slot_id, F32(0.0)).astype(BF16)
    place = jnp.where(
        jnp.broadcast_to(slotv[...], (slots, slots)) == lax.broadcasted_iota(I32, (slots, slots), 0),
        F32(1.0),
        F32(0.0),
    ).astype(BF16)
    taken_from = nt_dot(route, place).astype(I32)

    cells_done.wait()
    total = lax.fori_loop(0, first_steps, gather_sums, jnp.zeros((high_count, 8 * LO), F32))
    pl.when(idle)(lambda: spread_sums(total))

    pl.semaphore_wait(barrier, count)
    def answer(o, vector):
        pl.semaphore_signal(ready.at[0], inc=1, device_id=device(vector), device_id_type=MESH)

    answer_far = functools.partial(answer, block_id(BEFORE), BEFORE)
    if split:
        pl.when(alone_down)(lambda: each_neighbour(answer, levels=(-1,)))
        pl.when(exists(BEFORE) & jnp.logical_not(alone_down))(answer_far)
    else:
        pl.when(exists(BEFORE))(answer_far)
    each_neighbour(lambda o, v: record_copy(o, v).start(), BEYOND, not_up)

    total = lax.fori_loop(first_steps, steps, gather_sums, total)
    pl.when(jnp.logical_not(idle))(lambda: spread_sums(total))

    def force_copy(o, vector):
        return pltpu.make_async_remote_copy(
            src_ref=fsend.at[o], dst_ref=frecv.at[26 - o], send_sem=sent.at[0],
            recv_sem=forces_in.at[0], device_id=device(vector), device_id_type=MESH,
        )

    each_neighbour(lambda o, v: force_copy(o, v).start(), BEYOND, not_up)

    def dot(c, vec):
        value = None
        for axis in range(3):
            if c[axis]:
                term = vec[axis] if c[axis] == 1 else -vec[axis]
                value = term if value is None else value + term
        return value

    def collide_fluid(r):
        rows = pl.ds(pl.multiple_of(r * 8, 8), 8)
        rho = state[0, rows, :]
        u = [state[1 + d, rows, :] for d in range(3)]
        weight = state[4, rows, :]
        keep = (1.0 - weight) * (1.0 / RELAX_TIME)
        rest_u = 1.0 - 1.5 * (u[0] * u[0] + u[1] * u[1] + u[2] * u[2])
        scaled = {w: w * rho for w in sorted(set(WEIGHTS))}
        f0 = pv[0, rows, :]
        eq_u = scaled[WEIGHTS[0]] * rest_u
        rel[PLACE[0], rows, :] = f0 - keep * (f0 - eq_u) - weight * eq_u
        for i in range(1, 19, 2):
            j = OPPOSITE[i]
            share = scaled[WEIGHTS[i]]
            pu = dot(LATTICE[i], u)
            even = share * (rest_u + 4.5 * pu * pu)
            odd = share * (3.0 * pu)
            fi, fj = pv[i, rows, :], pv[j, rows, :]
            ui, uj = even + odd, even - odd
            diff = fj - fi
            rel[PLACE[i], rows, :] = fi - keep * (fi - ui) + weight * (diff - uj)
            rel[PLACE[j], rows, :] = fj - keep * (fj - uj) - weight * (diff + ui)

    def collide_some(step, carry):
        for n in range(COLLIDE_UNROLL):
            collide_fluid(step * COLLIDE_UNROLL + n)
        return carry

    lax.fori_loop(0, chunks // COLLIDE_UNROLL, collide_some, 0)

    edges = {(axis, sign): n for n, (axis, sign) in enumerate([(1, 1), (1, -1), (2, 1), (2, -1)])}
    edge_index, edge_share, line_of = {}, {}, {}
    for sign in (1, -1):
        line = pl.ds(Y - 1 if sign == 1 else 0, X, stride=Y)
        for entry, i in enumerate(LEAVING[1, sign]):
            ypack[side(sign), entry] = rel[PLACE[i], line, :]
        line_of[sign] = line

    def pack_columns(read, entries, edge, start):
        packed = start
        for entry in range(entries):
            for r in range(chunks):
                column = entry * chunks + r
                turned = read(entry, pl.ds(r * 8, 8))
                if (column - edge) % Z:
                    turned = pltpu.roll(turned, (column - edge) % Z, 1)
                packed = jnp.where(lane8 == column, turned, packed)
        return packed

    repeat = lax.rem(lane8, chunks)
    for sign in (1, -1):
        edge = Z - 1 if sign == 1 else 0
        leaving = LEAVING[2, sign]
        zpack[side(sign)] = pack_columns(
            lambda entry, rows: rel[PLACE[leaving[entry]], rows, :], 5, edge, jnp.zeros((8, Z), F32)
        )
        share = pack_columns(lambda entry, rows: state[5, rows, :], 1, edge, jnp.zeros((8, Z), F32))
        index = pack_columns(
            lambda entry, rows: iv[rows, :], 1, edge, jnp.full((8, Z), touches, I32)
        )
        edge_share[sign] = lane_take(share, repeat)
        edge_index[sign] = lane_take(index, repeat)

    def reach_far():
        pl.semaphore_wait(ready.at[0], 1)
        record_copy(block_id(BEYOND), BEYOND).start()
        force_copy(block_id(BEYOND), BEYOND).start()

    def reach_up():
        pl.semaphore_wait(ready.at[0], plane)
        each_neighbour(lambda o, v: record_copy(o, v).start(), levels=(1,))
        each_neighbour(lambda o, v: force_copy(o, v).start(), levels=(1,))

    if split:
        pl.when(alone_up)(reach_up)
        pl.when(exists(BEYOND) & jnp.logical_not(alone_up))(reach_far)
    else:
        pl.when(exists(BEYOND))(reach_far)
    wait_rows(record_rows, recs_in)

    def place_of(index):
        block = lax.shift_right_logical(index, slots.bit_length() - 1)
        return block, index - block * slots

    def wide(o, row):
        return jnp.broadcast_to(recs[o, row], (8, Z))

    index_rows = [touch_row[:, g * Z : (g + 1) * Z] for g in range(groups)]
    unused = [jnp.full((8 - 3 * groups, Z), 27 * slots, I32)] if groups * 3 < 8 else []
    touch_blocks, touch_local = place_of(jnp.concatenate(index_rows * 3 + unused, axis=0))
    found = jnp.zeros((8, Z), F32)
    for o in blocks:
        rows = jnp.where(sub8 < groups, wide(o, 3), jnp.where(sub8 < 2 * groups, wide(o, 4), wide(o, 5)))
        found = jnp.where(touch_blocks == o, lane_take(rows, touch_local), found)
    found = SPEED_UNIT * found
    tables = [
        [jnp.broadcast_to(found[d * groups + g][None], (8, Z)) for g in range(groups)]
        for d in range(3)
    ]

    def solid_velocity(index):
        group = lax.shift_right_logical(index, Z.bit_length() - 1)
        local = index - group * Z
        v = []
        for d in range(3):
            value = jnp.zeros((8, Z), F32)
            for g in range(groups):
                value = jnp.where(group == g, lane_take(tables[d][g], local), value)
            v.append(value)
        return v, 1.0 - 1.5 * (v[0] * v[0] + v[1] * v[1] + v[2] * v[2])

    def halo_copy(vector):
        if vector[2] != 0 and vector[1] != 0:
            row = pl.ds((Y - 1) % 8 if vector[1] == 1 else 0, 1)
            src, dst = zpack.at[side(vector[2]), row], thalo.at[TILE_ID[vector], row]
        elif vector[2] != 0:
            src, dst = zpack.at[side(vector[2])], thalo.at[TILE_ID[vector]]
        elif vector[0] != 0 and vector[1] != 0:
            entry = LEAVING[1, vector[1]].index(LATTICE.index(vector))
            row = pl.ds(X - 1 if vector[0] == 1 else 0, 1)
            src, dst = ypack.at[side(vector[1]), entry, row], thalo.at[TILE_ID[vector], row]
        elif vector[0] != 0:
            start = 5 * side(vector[0])
            row = (X - 1) * Y if vector[0] == 1 else 0
            src = rel.at[pl.ds(start, 5), pl.ds(row, Y), :]
            dst = xhalo.at[side(vector[0])]
        else:
            src, dst = ypack.at[side(vector[1])], yhalo.at[side(vector[1])]
        return pltpu.make_async_remote_copy(
            src_ref=src, dst_ref=dst, send_sem=sent.at[0], recv_sem=edges_in.at[0],
            device_id=device(vector), device_id_type=MESH,
        )

    def when_there(vector, action):
        pl.when(exists(vector))(action)

    entry8 = lane8 // chunks
    for sign in (1, -1):
        v, rest = solid_velocity(edge_index[sign])
        along = v[2] if sign == 1 else -v[2]
        base = jnp.zeros((8, Z), F32)
        for entry, i in enumerate(LEAVING[2, sign]):
            here = entry8 == entry
            base = jnp.where(here, F32(WEIGHTS[i]), base)
            for d in range(2):
                c = LATTICE[i][d]
                if c:
                    along = jnp.where(here, along + v[d] if c == 1 else along - v[d], along)
        zpack[side(sign)] = zpack[side(sign)] + edge_share[sign] * base * (
            rest + (4.5 * along + 3.0) * along
        )
    for vector in HALOS[::-1]:
        if vector[2] != 0:
            when_there(vector, lambda vector=vector: halo_copy(vector).start())
    for sign in (1, -1):
        v, rest = solid_velocity(iv[line_of[sign], :])
        share = state[5, line_of[sign], :]
        for entry, i in enumerate(LEAVING[1, sign]):
            along = dot(LATTICE[i], v)
            ypack[side(sign), entry] = ypack[side(sign), entry] + share * F32(WEIGHTS[i]) * (
                rest + (4.5 * along + 3.0) * along
            )
    for vector in HALOS[::-1]:
        if vector[2] == 0 and vector[1] != 0:
            when_there(vector, lambda vector=vector: halo_copy(vector).start())

    def collide_solid(r):
        rows = pl.ds(pl.multiple_of(r * 8, 8), 8)
        v, rest = solid_velocity(iv[rows, :])
        share = state[5, rows, :]
        scaled = {w: w * share for w in sorted(set(WEIGHTS))}
        rel[PLACE[0], rows, :] = rel[PLACE[0], rows, :] + scaled[WEIGHTS[0]] * rest
        for i in range(1, 19, 2):
            j = OPPOSITE[i]
            ps = dot(LATTICE[i], v)
            even = scaled[WEIGHTS[i]] * (rest + 4.5 * ps * ps)
            odd = scaled[WEIGHTS[i]] * (3.0 * ps)
            rel[PLACE[i], rows, :] = rel[PLACE[i], rows, :] + (even + odd)
            rel[PLACE[j], rows, :] = rel[PLACE[j], rows, :] + (even - odd)

    own = [recs[13, d] for d in range(6)]
    contact = [jnp.zeros((1, slots), F32) for _ in range(3)]
    spans = (X / R, Y / R, Z / R)
    for start in range(0, neighbours, 8):
        used = min(8, neighbours - start)
        lines = [cv[n] for n in range(start, start + used)]
        half = used <= 4
        if half:
            lines = (lines + [jnp.full((4 - used, slots), 27 * slots, I32)] * (used < 4)) * 2
        elif used < 8:
            lines.append(jnp.full((8 - used, slots), 27 * slots, I32))
        entries = jnp.concatenate(lines, axis=0)
        entry_block, local = place_of(entries)
        near = [jnp.zeros((8, slots), F32)] * (2 if half else 3)
        for o in blocks:
            hit = entry_block == o
            lines = [wide(o, d) for d in range(3)]
            if half:
                lines = [jnp.where(sub8 < 4, lines[0], lines[1]), lines[2]]
            near = [
                jnp.where(hit, lane_take(line, local), value) for line, value in zip(lines, near)
            ]
        if half:
            near = [near[0], pltpu.roll(near[0], 4, 0), near[1]]
        nine = jnp.zeros(entry_block.shape, I32)
        for step in (9, 18, 27):
            nine = nine + (entry_block >= step).astype(I32)
        inner = entry_block - 9 * nine
        three = (inner >= 3).astype(I32) + (inner >= 6).astype(I32)
        moves = (nine - 1, three - 1, inner - 3 * three - 1)
        apart = [
            jnp.broadcast_to(own[d], (8, slots)) - (near[d] + moves[d].astype(F32) * spans[d])
            for d in range(3)
        ]
        soften = 1.0 + 0.25 * (apart[0] * apart[0] + apart[1] * apart[1] + apart[2] * apart[2])
        valid = entries < 27 * slots
        if half:
            valid = valid & (sub8 < 4)
        strength = CONTACT_GAIN * valid.astype(F32) / (soften * soften)
        for d in range(3):
            contact[d] = contact[d] + jnp.sum(apart[d] * strength, axis=0, keepdims=True)

    wait_rows(force_rows, forces_in)
    force = fsend[13]
    for o in blocks:
        force = force + frecv[o]
    gravity = (0.0, 0.0, GRAVITY_STEP)
    velocity_new, position_new = [], []
    for d in range(3):
        speed = own[3 + d]
        hydro = force[d : d + 1] - force[3:4] * (SPEED_UNIT * speed)
        velocity = speed + FORCE_SCALE * hydro + contact[d] - gravity[d]
        velocity_new.append(velocity)
        position_new.append(own[d] + velocity * (SPEED_UNIT / R))
    record = jnp.concatenate(position_new + velocity_new + [jnp.zeros((2, slots), F32)], axis=0)

    def routed(n, vector):
        origin = jnp.broadcast_to(taken_from[n : n + 1], (8, slots))
        moved = lane_take(record, jnp.where(origin > 0, origin - 1, 0))
        shift = jnp.zeros((8, slots), F32)
        for d in range(3):
            if vector[d]:
                shift = jnp.where(row_id == d, F32(vector[d] * spans[d]), shift)
        return jnp.where(origin > 0, moved - shift, F32(0.0))

    def move_copy(n):
        return pltpu.make_async_remote_copy(
            src_ref=msend.at[n], dst_ref=mrecv.at[n], send_sem=sent.at[0],
            recv_sem=edges_in.at[0], device_id=device(FACES[n]), device_id_type=MESH,
        )

    for n, vector in enumerate(FACES):
        msend[n] = routed(n, vector)
        when_there(vector, lambda n=n: move_copy(n).start())
    stay = routed(6, (0, 0, 0))

    for x in sorted({0, X - 1}):
        for h in range(halves):
            collide_solid(x * halves + h)
    for vector in HALOS:
        if vector[1] == 0 and vector[2] == 0:
            when_there(vector, lambda vector=vector: halo_copy(vector).start())

    def collide_rest(step, carry):
        for n in range(SOLID_UNROLL):
            collide_solid(halves + step * SOLID_UNROLL + n)
        return carry

    lax.fori_loop(0, (X - 2) * halves // SOLID_UNROLL, collide_rest, 0)

    wait_rows(sent_rows, sent)
    wait_rows(edge_rows, edges_in)
    for n in range(len(FACES)):
        stay = stay + mrecv[n]
    for d in range(6):
        moved[d] = stay[d : d + 1]


def pass_kernel(sizes, shape, rel, xhalo, yhalo, thalo, moved, out_hbm, part_out, pv, out_sem):
    X, Y, Z = shape
    chunks = X * Y // 8
    halves = Y // 8
    me = tuple(lax.axis_index(a) for a in ("gx", "gy", "gz"))
    part_copy = pltpu.make_async_copy(moved, part_out, out_sem.at[1])
    part_copy.start()
    suby = lax.broadcasted_iota(I32, (Y, Z), 0)
    laney = lax.broadcasted_iota(I32, (Y, Z), 1)
    open_back = {
        (axis, sign): (me[axis] > 0) if sign == 1 else (me[axis] < sizes[axis] - 1)
        for axis in range(3)
        for sign in (1, -1)
    }
    target = {1: 0, -1: Z - 1}
    row_edge = {1: 0, -1: Y - 1}

    def edge_mask(c):
        mask = None
        if c[1]:
            blocked = jnp.broadcast_to(jnp.where(open_back[1, c[1]], -1, row_edge[c[1]]), (Y, Z))
            mask = suby != blocked
        if c[2]:
            blocked = jnp.broadcast_to(jnp.where(open_back[2, c[2]], -1, target[c[2]]), (Y, Z))
            other = laney != blocked
            mask = other if mask is None else mask & other
        return mask

    for i in PASS_ORDER:
        c = LATTICE[i]
        j = OPPOSITE[i]
        mask = edge_mask(c)
        for x in range(X):
            from_x = x - c[0]
            inside_x = 0 <= from_x < X
            wrapped = from_x % X
            if inside_x:
                slab = rel[PLACE[i], from_x * Y : (from_x + 1) * Y, :]
            else:
                slab = xhalo[side(c[0]), LEAVING[0, c[0]].index(i)]
            turn = 1 if c[2] == 1 else Z - 1
            if c[2]:
                entry = LEAVING[2, c[2]].index(i)
                tile = thalo[TILE_ID[(0, 0, c[2])]] if inside_x else thalo[TILE_ID[(c[0], 0, c[2])]]
                columns = []
                for h in range(halves):
                    column = entry * chunks + wrapped * halves + h
                    amount = (target[c[2]] - column) % Z
                    columns.append(pltpu.roll(tile, amount, 1) if amount else tile)
                edge_columns = jnp.concatenate(columns, axis=0)
                slab = jnp.where(laney == target[c[2]], edge_columns, pltpu.roll(slab, turn, 1))
            if c[1]:
                entry = LEAVING[1, c[1]].index(i)
                if inside_x:
                    line = yhalo[side(c[1]), entry, from_x : from_x + 1, :]
                else:
                    line = thalo[TILE_ID[(c[0], c[1], 0)], wrapped : wrapped + 1, :]
                if c[2]:
                    entry = LEAVING[2, c[2]].index(i)
                    last = (Y - 1) if c[1] == 1 else 0
                    column = entry * chunks + from_x * halves + last // 8
                    amount = (target[c[2]] - column) % Z
                    tile = thalo[TILE_ID[c]]
                    tile = pltpu.roll(tile, amount, 1) if amount else tile
                    corner = tile[last % 8 : last % 8 + 1]
                    tile = yhalo[side(c[1]), LEAVING[1, c[1]].index(i)]
                    line = pltpu.roll(tile, turn, 1)[from_x : from_x + 1]
                    line = jnp.where(laney[0:1] == target[c[2]], corner, line)
                slab = pltpu.roll(slab, 1 if c[1] == 1 else Y - 1, 0)
                slab = jnp.where(suby == row_edge[c[1]], jnp.broadcast_to(line, (Y, Z)), slab)
            mirror = rel[PLACE[j], x * Y : (x + 1) * Y, :] if c != (0, 0, 0) else None
            if mask is not None:
                slab = jnp.where(mask, slab, mirror)
            if not inside_x:
                closed = jnp.broadcast_to(open_back[0, c[0]].astype(I32), (Y, Z))
                slab = jnp.where(closed > 0, slab, mirror)
            pv[i, x * Y : (x + 1) * Y, :] = slab
        pltpu.make_async_copy(pv.at[i], out_hbm.at[i], out_sem.at[0]).start()

    part_copy.wait()
    pltpu.make_async_copy(pv, out_hbm, out_sem.at[0]).wait()


def body(sizes, populations, solid_fraction, intersection, touch, particles, contacts, dest_code, dest_slot):
    count, X, Y, Z = populations.shape
    slots = particles.shape[4]
    touches = touch.shape[3]
    neighbours = contacts.shape[3]
    any_space = pl.BlockSpec(memory_space=pl.ANY)
    dma = pltpu.SemaphoreType.DMA
    vmem = pl.BlockSpec(memory_space=pltpu.VMEM)
    values = (
        populations.reshape(count, X * Y, Z),
        solid_fraction.reshape(X * Y, Z),
        intersection.reshape(X * Y, Z),
        touch.reshape(1, touches),
        particles.reshape(6, 1, slots),
        contacts.reshape(neighbours, 1, slots),
        dest_code.reshape(1, slots),
        dest_slot.reshape(1, slots),
    )
    handed = pl.pallas_call(
        functools.partial(kernel, sizes, (X, Y, Z)),
        out_shape=(
            pltpu.VMEM((count, X * Y, Z), F32),
            pltpu.VMEM((2, 5, Y, Z), F32),
            pltpu.VMEM((2, 5, X, Z), F32),
            pltpu.VMEM((len(TILES), 8, Z), F32),
            pltpu.VMEM((6, 1, slots), F32),
        ),
        in_specs=[pl.BlockSpec(memory_space=pltpu.HBM)] * 8,
        out_specs=(vmem,) * 5,
        scratch_shapes=[
            pltpu.VMEM((count, X * Y, Z), F32),
            pltpu.VMEM((X * Y, Z), F32),
            pltpu.VMEM((X * Y, Z), I32),
            pltpu.VMEM((1, touches), I32),
            pltpu.VMEM((neighbours, 1, slots), I32),
            pltpu.VMEM((1, slots), I32),
            pltpu.VMEM((1, slots), I32),
            pltpu.VMEM((27, 6, 1, slots), F32),
            pltpu.VMEM((6, X * Y, Z), F32),
            pltpu.VMEM((touches // LO, Z), F32),
            pltpu.VMEM((27, 4, slots), F32),
            pltpu.VMEM((27, 4, slots), F32),
            pltpu.VMEM((2, 5, X, Z), F32),
            pltpu.VMEM((2, 8, Z), F32),
            pltpu.VMEM((len(FACES), 8, slots), F32),
            pltpu.VMEM((len(FACES), 8, slots), F32),
            pltpu.VMEM((slots, touches), BF16),
            pltpu.VMEM((26 * 10 + 10 * (X + Y) + 8 * (len(TILES) + len(FACES)), Z), F32),
            dma((2 + X * Y // (8 * SUM_UNROLL),)),
            dma((1,)),
            dma((1,)),
            dma((1,)),
            dma((1,)),
            pltpu.SemaphoreType.REGULAR((1,)),
        ],
        compiler_params=pltpu.CompilerParams(
            collective_id=0, has_side_effects=True, vmem_limit_bytes=GRANT
        ),
    )(*[pltpu.with_memory_space_constraint(value, pltpu.HBM) for value in values])
    out, moved = pl.pallas_call(
        functools.partial(pass_kernel, sizes, (X, Y, Z)),
        out_shape=(
            jax.ShapeDtypeStruct((count, X * Y, Z), F32),
            jax.ShapeDtypeStruct((6, 1, slots), F32),
        ),
        in_specs=[vmem] * 5,
        out_specs=(any_space, any_space),
        scratch_shapes=[pltpu.VMEM((count, X * Y, Z), F32), dma((2,))],
        compiler_params=pltpu.CompilerParams(vmem_limit_bytes=GRANT),
    )(*[pltpu.with_memory_space_constraint(value, pltpu.VMEM) for value in handed])
    return (out.reshape(count, X, Y, Z), moved.reshape(1, 1, 1, 6, slots))


def solution(mesh):
    placed = (
        P(None, "gx", "gy", "gz"),
        P("gx", "gy", "gz"),
        P("gx", "gy", "gz"),
        P("gx", "gy", "gz", None),
        P("gx", "gy", "gz", None, None),
        P("gx", "gy", "gz", None, None),
        P("gx", "gy", "gz", None),
        P("gx", "gy", "gz", None),
    )
    sizes = tuple(mesh.shape[axis] for axis in ("gx", "gy", "gz"))
    return jax.shard_map(
        functools.partial(body, sizes),
        mesh=mesh,
        in_specs=placed,
        out_specs=(P(None, "gx", "gy", "gz"), P("gx", "gy", "gz", None, None)),
        check_vma=False,
    )
```

```python
import functools
import itertools

import jax
import jax.numpy as jnp
from jax import lax
from jax.experimental import pallas as pl
from jax.experimental.pallas import tpu as pltpu
from jax.sharding import PartitionSpec as P

R = 8

LATTICE = [
    (0, 0, 0),
    (1, 0, 0),
    (-1, 0, 0),
    (0, 1, 0),
    (0, -1, 0),
    (0, 0, 1),
    (0, 0, -1),
    (1, 1, 0),
    (-1, -1, 0),
    (1, -1, 0),
    (-1, 1, 0),
    (1, 0, 1),
    (-1, 0, -1),
    (1, 0, -1),
    (-1, 0, 1),
    (0, 1, 1),
    (0, -1, -1),
    (0, 1, -1),
    (0, -1, 1),
]
OPPOSITE = [0, 2, 1, 4, 3, 6, 5, 8, 7, 10, 9, 12, 11, 14, 13, 16, 15, 18, 17]
WEIGHTS = [1.0 / 3.0] + [1.0 / 18.0] * 6 + [1.0 / 36.0] * 12
RELAX_TIME = 0.8
SPEED_UNIT = 0.05
FORCE_SCALE = 0.1
CONTACT_GAIN = 1.0
GRAVITY_STEP = 0.1

MESH = pl.DeviceIdType.MESH
F32 = jnp.float32
BF16 = jnp.bfloat16
I32 = jnp.int32

LEAVING = {
    (axis, sign): [i for i, c in enumerate(LATTICE) if c[axis] == sign]
    for axis in range(3)
    for sign in (1, -1)
}
ORDER = LEAVING[0, 1] + LEAVING[0, -1] + [i for i, c in enumerate(LATTICE) if c[0] == 0]
PLACE = {i: n for n, i in enumerate(ORDER)}
HALOS = [c for c in LATTICE if c != (0, 0, 0)]
HALO_ID = {c: n for n, c in enumerate(HALOS)}
PASS_ORDER = sorted(range(19), key=lambda i: (LATTICE[i][2] != 0, i))
TILES = [c for c in HALOS if c[2] != 0] + [c for c in HALOS if c[2] == 0 and c[0] != 0 and c[1] != 0]
TILE_ID = {c: n for n, c in enumerate(TILES)}
FACES = [(1, 0, 0), (-1, 0, 0), (0, 1, 0), (0, -1, 0), (0, 0, 1), (0, 0, -1)]
LO = 8
GRANT = 16 * 2**20
SUM_UNROLL = 8
EARLY_STEPS = 1
COLLIDE_UNROLL = 2
SOLID_UNROLL = 8
BEYOND = (1, 1, 1)
BEFORE = (-1, -1, -1)


def block_id(vector):
    return 9 * (vector[0] + 1) + 3 * (vector[1] + 1) + vector[2] + 1


def side(sign):
    return 0 if sign == 1 else 1


def lane_take(table, index):
    return jnp.take_along_axis(table, index, axis=1, mode="promise_in_bounds")


def nt_dot(left, right):
    return lax.dot_general(left, right, (((1,), (1,)), ((), ())), preferred_element_type=F32)


def split_pair(value):
    high = value.astype(BF16).astype(F32)
    return high, value - high


def kernel(
    sizes,
    shape,
    pops_hbm, frac_hbm, inter_hbm, touch_hbm, part_hbm, cont_hbm, code_hbm, slot_hbm,
    rel, xhalo, yhalo, thalo, moved,
    pv, fv, iv, tv, cv, codev, slotv,
    recs, state, sums, fsend, frecv, ypack, zpack, msend, mrecv,
    picked, ruler, xpack, in_sem, sent, recs_in, forces_in, edges_in, ready,
):
    X, Y, Z = shape
    slots = recs.shape[3]
    touches = tv.shape[1]
    neighbours = cv.shape[0]
    chunks = X * Y // 8
    halves = Y // 8
    me = tuple(lax.axis_index(a) for a in ("gx", "gy", "gz"))

    cell_ins = [
        pltpu.make_async_copy(inter_hbm, iv, in_sem.at[1]),
        pltpu.make_async_copy(frac_hbm, fv, in_sem.at[1]),
    ]
    small_ins = [
        pltpu.make_async_copy(src, dst, in_sem.at[0])
        for src, dst in [
            (part_hbm, recs.at[13]), (touch_hbm, tv), (cont_hbm, cv), (code_hbm, codev),
            (slot_hbm, slotv),
        ]
    ]
    small_rows = (touches + (neighbours + 8) * slots) // Z
    cells_done = pltpu.make_async_copy(pops_hbm.at[0:2], pv.at[0:2], in_sem.at[1])
    small_done = pltpu.make_async_copy(
        pops_hbm.at[0, 0:small_rows], pv.at[0, 0:small_rows], in_sem.at[0]
    )
    steps = chunks // SUM_UNROLL
    span = SUM_UNROLL * 8

    def pops_in(step):
        rows = pl.ds(pl.multiple_of(step * span, span), span)
        return pltpu.make_async_copy(pops_hbm.at[:, rows], pv.at[:, rows], in_sem.at[2 + step])

    there = {
        (axis, sign): (me[axis] < sizes[axis] - 1) if sign == 1 else (me[axis] > 0)
        for axis in range(3)
        for sign in (1, -1)
    }

    def exists(vector):
        flags = [there[axis, step] for axis, step in enumerate(vector) if step]
        return functools.reduce(lambda p, q: p & q, flags)

    def device(vector):
        return tuple(position + step for position, step in zip(me, vector))

    def steps_along(axis):
        if sizes[axis] == 1:
            return [((0,), None)]
        if sizes[axis] == 2:
            return [((0, 1 - 2 * me[axis]), None)]
        return [((-1,), there[axis, -1]), ((0,), None), ((1,), there[axis, 1])]

    def far(vector):
        return sum(1 for step in vector if not (isinstance(step, int) and step == 0))

    def each_neighbour(action, skip=(2, 2, 2), allow={}, levels=(-1, 0, 1)):
        groups = []
        for choice in itertools.product(*[steps_along(axis) for axis in range(3)]):
            level = choice[2][0][0]
            if sizes[2] > 2 and level not in levels:
                continue
            flags = [flag for _, flag in choice if flag is not None]
            if level in allow:
                flags.append(allow[level])
            vectors = list(itertools.product(*[values for values, _ in choice]))
            groups.append((flags, sorted([v for v in vectors if far(v)], key=far, reverse=True)))

        def act(vectors):
            for vector in vectors:
                do = functools.partial(action, block_id(vector), vector)
                pairs = list(zip(range(3), vector, skip))
                fixed = [p for p in pairs if isinstance(p[1], int)]
                moving = [p for p in pairs if not isinstance(p[1], int)]
                if any(step != other for _, step, other in fixed) or 2 in skip:
                    do()
                elif moving and all(other for _, _, other in moving):
                    apart = [jnp.logical_not(there[axis, other]) for axis, _, other in moving]
                    pl.when(functools.reduce(lambda p, q: p | q, apart))(do)
                elif moving:
                    do()

        for flags, vectors in sorted(groups, key=lambda g: max(map(far, g[1]), default=0), reverse=True):
            run = functools.partial(act, vectors)
            if flags:
                pl.when(functools.reduce(lambda p, q: p & q, flags))(run)
            else:
                run()

    windows = [
        [0] if size == 1 else [0 - at, 1 - at] if size == 2 else [-1, 0, 1]
        for size, at in zip(sizes, me)
    ]
    blocks = [block_id((x, y, z)) for x in windows[0] for y in windows[1] for z in windows[2]]

    barrier = pltpu.get_barrier_semaphore()

    half = sizes[2] // 2
    split = sizes[2] > 2
    alone_up = there[2, 1] & (me[2] >= half)
    alone_down = me[2] > half
    not_up = {1: jnp.logical_not(alone_up)} if split else {}
    not_down = {-1: jnp.logical_not(alone_down)} if split else {}

    def greet(o, vector):
        pl.semaphore_signal(barrier, inc=1, device_id=device(vector), device_id_type=MESH)

    for copy in small_ins:
        copy.start()
    pops_in(0).start()
    for copy in cell_ins:
        copy.start()
    for step in range(1, steps):
        pops_in(step).start()
    each_neighbour(greet, BEFORE, not_down)

    around = [
        (me[axis] > 0).astype(I32) + (me[axis] < sizes[axis] - 1).astype(I32) for axis in range(3)
    ]
    options = [[0] if size == 1 else [1] if size == 2 else [1, 2] for size in sizes]
    nearby = lambda n: (n[0] + 1) * (n[1] + 1) * (n[2] + 1) - 1
    record_rows = lambda n: 6 * nearby(n)
    force_rows = lambda n: 4 * nearby(n)

    def edge_rows(n):
        x, y, z = n
        tiles = 8 * (z + x * z + x + y + z) + x * y + y * z
        return 5 * (Y * x + X * y) + tiles

    sent_rows = lambda n: record_rows(n) + force_rows(n) + edge_rows(n)

    plane = (around[0] + 1) * (around[1] + 1)
    waiting = exists(BEYOND).astype(I32)
    if split:
        waiting = jnp.where(alone_up, plane, waiting)
    count = nearby(around) - waiting

    def wait_rows(measure, semaphore):
        amount = measure(around)
        for rows in sorted({measure(n) for n in itertools.product(*options)}):
            if rows:
                part = ruler.at[0:rows]
                copy = pltpu.make_async_copy(part, part, semaphore.at[0])
                pl.when(amount == rows)(copy.wait)

    def record_copy(o, vector):
        return pltpu.make_async_remote_copy(
            src_ref=recs.at[13], dst_ref=recs.at[26 - o], send_sem=sent.at[0],
            recv_sem=recs_in.at[0], device_id=device(vector), device_id_type=MESH,
        )

    sub8 = lax.broadcasted_iota(I32, (8, Z), 0)
    lane8 = lax.broadcasted_iota(I32, (8, Z), 1)
    high_count = touches // LO
    sub_high = lax.broadcasted_iota(I32, (high_count, Z), 0)

    def gather_pieces(r):
        rows = pl.ds(pl.multiple_of(r * 8, 8), 8)
        f = [pv[i, rows, :] for i in range(19)]
        rho = functools.reduce(lambda a, b: a + b, f)
        momentum = []
        for axis in range(3):
            terms = None
            for i in LEAVING[axis, 1]:
                diff = f[i] - f[OPPOSITE[i]]
                terms = diff if terms is None else terms + diff
            momentum.append(terms)
        index = iv[rows, :]
        eps = fv[rows, :]
        weight = jnp.where(
            index < touches,
            eps * (RELAX_TIME - 0.5) / (1.0 - eps + (RELAX_TIME - 0.5)),
            F32(0.0),
        )
        inverse = 1.0 / rho
        state[0, rows, :] = rho
        for axis in range(3):
            state[1 + axis, rows, :] = momentum[axis] * inverse
        state[4, rows, :] = weight
        wanted = [weight * m for m in momentum] + [weight * rho]
        state[5, rows, :] = wanted[3]
        pairs = [split_pair(w) for w in wanted]
        pieces = [p[0] for p in pairs] + [p[1] for p in pairs]
        high = index // LO if LO & (LO - 1) else lax.shift_right_logical(index, LO.bit_length() - 1)
        low = index - high * LO
        return pieces, high, low

    def gather_pairs(pieces, high, low):
        left, right = [], []
        for row in range(8):
            high_row = jnp.broadcast_to(high[row : row + 1], (high_count, Z))
            match = jnp.broadcast_to(low[row : row + 1], (8, Z)) == sub8
            left.append(jnp.where(high_row == sub_high, F32(1.0), F32(0.0)).astype(BF16))
            right.append(
                jnp.concatenate(
                    [
                        jnp.where(match, jnp.broadcast_to(pieces[p][row : row + 1], (8, Z)), F32(0.0))
                        for p in range(8)
                    ],
                    axis=0,
                ).astype(BF16)
            )
        return right, left

    def gather_sums(step, total):
        pops_in(step).wait()
        right, left = [], []
        for n in range(SUM_UNROLL):
            more_right, more_left = gather_pairs(*gather_pieces(step * SUM_UNROLL + n))
            right += more_right
            left += more_left
        return total + nt_dot(jnp.concatenate(left, axis=1), jnp.concatenate(right, axis=1))

    groups = touches // Z

    def spread_sums(total):
        sums[:, 0 : 8 * LO] = total
        both = sums[...]
        lane_high = lax.shift_right_logical(lane8, LO.bit_length() - 1)
        lane_low = lane8 - lane_high * LO
        parts = []
        for g in range(groups):
            lines = []
            for q in range(4):
                line = jnp.zeros((8, Z), F32)
                for part in range(Z // (8 * LO)):
                    first_row = g * (Z // LO) + part * 8
                    rows = both[first_row : first_row + 8]
                    taken = lane_take(rows, q * LO + lane_low)
                    taken = taken + lane_take(rows, (4 + q) * LO + lane_low)
                    line = line + jnp.where(sub8 + part * 8 == lane_high, taken, F32(0.0))
                lines.append(jnp.sum(line, axis=0, keepdims=True))
            quad = jnp.concatenate(lines, axis=0)
            first, second = split_pair(quad)
            parts.append((first, second))
        tables = [
            jnp.concatenate([jnp.concatenate([part[h]] * 2, axis=0) for part in parts], axis=1)
            for h in range(2)
        ]
        block8 = jnp.broadcast_to(touch_block, (8, touches))
        upper = lax.broadcasted_iota(I32, (8, touches), 0) < 4
        lefts = []
        for n in range(0, len(blocks), 2):
            hit = block8 == jnp.where(upper, blocks[n], blocks[min(n + 1, len(blocks) - 1)])
            lefts.append(
                jnp.concatenate([jnp.where(hit, table, F32(0.0)) for table in tables], axis=1)
            )
        spread = nt_dot(jnp.concatenate(lefts, axis=0).astype(BF16), picked[...])
        for n, o in enumerate(blocks):
            fsend[o] = spread[4 * n : 4 * n + 4]

    middle = (lax.rem(me[0], 2) == 1) & there[0, 1]
    idle = (there[1, 1] & there[2, 1]) | (middle & (there[1, 1] | there[2, 1]))
    if split:
        idle = jnp.where(me[2] < half, idle, middle & there[1, 1])
    first_steps = jnp.where(idle, steps, EARLY_STEPS)
    if split:
        last_y = jnp.logical_not(there[1, 1])
        top = jnp.logical_not(there[2, 1])
        first_steps = jnp.where((me[2] >= half) & (last_y | top), 0, first_steps)
        first_steps = jnp.where((me[2] >= half) & middle, jnp.where(last_y, 1, steps), first_steps)
    sums[...] = jnp.zeros(sums.shape, F32)
    frecv[13] = jnp.zeros(frecv.shape[1:], F32)

    def clear(ids):
        for o in ids:
            recs[o] = jnp.zeros(recs.shape[1:], F32)
            frecv[o] = jnp.zeros(frecv.shape[1:], F32)

    for choice in itertools.product(*[steps_along(axis) for axis in range(3)]):
        flags = [flag for _, flag in choice if flag is not None]
        if flags:
            ids = [block_id(vector) for vector in itertools.product(*[values for values, _ in choice])]
            present = functools.reduce(lambda p, q: p & q, flags)
            pl.when(jnp.logical_not(present))(functools.partial(clear, ids))
    for n, vector in enumerate(FACES):
        back = tuple(-step for step in vector)

        def clear_moved(n=n):
            mrecv[n] = jnp.zeros(mrecv.shape[1:], F32)

        pl.when(jnp.logical_not(exists(back)))(clear_moved)

    small_done.wait()
    touch_row = tv[...]
    touch_block = lax.shift_right_logical(touch_row, slots.bit_length() - 1)
    touch_slot = touch_row - touch_block * slots
    chosen = jnp.where(
        jnp.broadcast_to(touch_slot, (slots, touches))
        == lax.broadcasted_iota(I32, (slots, touches), 0),
        F32(1.0),
        F32(0.0),
    ).astype(BF16)
    picked[:, 0:touches] = chosen
    picked[:, touches : 2 * touches] = chosen

    pl.when(first_steps > 0)(cells_done.wait)
    total = lax.fori_loop(0, first_steps, gather_sums, jnp.zeros((high_count, 8 * LO), F32))
    pl.when(idle)(lambda: spread_sums(total))

    pl.semaphore_wait(barrier, count)
    def answer(o, vector):
        pl.semaphore_signal(ready.at[0], inc=1, device_id=device(vector), device_id_type=MESH)

    answer_far = functools.partial(answer, block_id(BEFORE), BEFORE)
    if split:
        pl.when(alone_down)(lambda: each_neighbour(answer, levels=(-1,)))
        pl.when(exists(BEFORE) & jnp.logical_not(alone_down))(answer_far)
    else:
        pl.when(exists(BEFORE))(answer_far)
    each_neighbour(lambda o, v: record_copy(o, v).start(), BEYOND, not_up)

    pl.when(first_steps == 0)(cells_done.wait)
    total = lax.fori_loop(first_steps, steps, gather_sums, total)
    pl.when(jnp.logical_not(idle))(lambda: spread_sums(total))

    def force_copy(o, vector):
        return pltpu.make_async_remote_copy(
            src_ref=fsend.at[o], dst_ref=frecv.at[26 - o], send_sem=sent.at[0],
            recv_sem=forces_in.at[0], device_id=device(vector), device_id_type=MESH,
        )

    each_neighbour(lambda o, v: force_copy(o, v).start(), BEYOND, not_up)

    code = codev[...]
    wanted_codes = [9 * (v[0] + 1) + 3 * (v[1] + 1) + v[2] + 1 for v in FACES] + [13]
    slot_id = lax.broadcasted_iota(I32, (8, slots), 1).astype(F32) + 1.0
    code_of = jnp.full((8, slots), 27, I32)
    row_id = lax.broadcasted_iota(I32, (8, slots), 0)
    for n, c in enumerate(wanted_codes):
        code_of = jnp.where(row_id == n, c, code_of)
    route = jnp.where(jnp.broadcast_to(code, (8, slots)) == code_of, slot_id, F32(0.0)).astype(BF16)
    place = jnp.where(
        jnp.broadcast_to(slotv[...], (slots, slots)) == lax.broadcasted_iota(I32, (slots, slots), 0),
        F32(1.0),
        F32(0.0),
    ).astype(BF16)
    taken_from = nt_dot(route, place).astype(I32)

    def dot(c, vec):
        value = None
        for axis in range(3):
            if c[axis]:
                term = vec[axis] if c[axis] == 1 else -vec[axis]
                value = term if value is None else value + term
        return value

    def collide_fluid(r):
        rows = pl.ds(pl.multiple_of(r * 8, 8), 8)
        rho = state[0, rows, :]
        u = [state[1 + d, rows, :] for d in range(3)]
        weight = state[4, rows, :]
        keep = (1.0 - weight) * (1.0 / RELAX_TIME)
        rest_u = 1.0 - 1.5 * (u[0] * u[0] + u[1] * u[1] + u[2] * u[2])
        scaled = {w: w * rho for w in sorted(set(WEIGHTS))}
        f0 = pv[0, rows, :]
        eq_u = scaled[WEIGHTS[0]] * rest_u
        rel[PLACE[0], rows, :] = f0 - keep * (f0 - eq_u) - weight * eq_u
        for i in range(1, 19, 2):
            j = OPPOSITE[i]
            share = scaled[WEIGHTS[i]]
            pu = dot(LATTICE[i], u)
            even = share * (rest_u + 4.5 * pu * pu)
            odd = share * (3.0 * pu)
            fi, fj = pv[i, rows, :], pv[j, rows, :]
            ui, uj = even + odd, even - odd
            diff = fj - fi
            rel[PLACE[i], rows, :] = fi - keep * (fi - ui) + weight * (diff - uj)
            rel[PLACE[j], rows, :] = fj - keep * (fj - uj) - weight * (diff + ui)

    def collide_some(step, carry):
        for n in range(COLLIDE_UNROLL):
            collide_fluid(step * COLLIDE_UNROLL + n)
        return carry

    lax.fori_loop(0, chunks // COLLIDE_UNROLL, collide_some, 0)

    edges = {(axis, sign): n for n, (axis, sign) in enumerate([(1, 1), (1, -1), (2, 1), (2, -1)])}
    edge_index, edge_share, line_of = {}, {}, {}
    for sign in (1, -1):
        line = pl.ds(Y - 1 if sign == 1 else 0, X, stride=Y)
        for entry, i in enumerate(LEAVING[1, sign]):
            ypack[side(sign), entry] = rel[PLACE[i], line, :]
        line_of[sign] = line

    def pack_columns(read, entries, edge, start):
        packed = start
        for entry in range(entries):
            for r in range(chunks):
                column = entry * chunks + r
                turned = read(entry, pl.ds(r * 8, 8))
                if (column - edge) % Z:
                    turned = pltpu.roll(turned, (column - edge) % Z, 1)
                packed = jnp.where(lane8 == column, turned, packed)
        return packed

    repeat = lax.rem(lane8, chunks)
    for sign in (1, -1):
        edge = Z - 1 if sign == 1 else 0
        leaving = LEAVING[2, sign]
        zpack[side(sign)] = pack_columns(
            lambda entry, rows: rel[PLACE[leaving[entry]], rows, :], 5, edge, jnp.zeros((8, Z), F32)
        )
        share = pack_columns(lambda entry, rows: state[5, rows, :], 1, edge, jnp.zeros((8, Z), F32))
        index = pack_columns(
            lambda entry, rows: iv[rows, :], 1, edge, jnp.full((8, Z), touches, I32)
        )
        edge_share[sign] = lane_take(share, repeat)
        edge_index[sign] = lane_take(index, repeat)

    def reach_far():
        pl.semaphore_wait(ready.at[0], 1)
        record_copy(block_id(BEYOND), BEYOND).start()
        force_copy(block_id(BEYOND), BEYOND).start()

    def reach_up():
        pl.semaphore_wait(ready.at[0], plane)
        each_neighbour(lambda o, v: record_copy(o, v).start(), levels=(1,))
        each_neighbour(lambda o, v: force_copy(o, v).start(), levels=(1,))

    if split:
        pl.when(alone_up)(reach_up)
        pl.when(exists(BEYOND) & jnp.logical_not(alone_up))(reach_far)
    else:
        pl.when(exists(BEYOND))(reach_far)
    wait_rows(record_rows, recs_in)

    def place_of(index):
        block = lax.shift_right_logical(index, slots.bit_length() - 1)
        return block, index - block * slots

    def wide(o, row):
        return jnp.broadcast_to(recs[o, row], (8, Z))

    index_rows = [touch_row[:, g * Z : (g + 1) * Z] for g in range(groups)]
    unused = [jnp.full((8 - 3 * groups, Z), 27 * slots, I32)] if groups * 3 < 8 else []
    touch_blocks, touch_local = place_of(jnp.concatenate(index_rows * 3 + unused, axis=0))
    found = jnp.zeros((8, Z), F32)
    for o in blocks:
        rows = jnp.where(sub8 < groups, wide(o, 3), jnp.where(sub8 < 2 * groups, wide(o, 4), wide(o, 5)))
        found = jnp.where(touch_blocks == o, lane_take(rows, touch_local), found)
    found = SPEED_UNIT * found
    tables = [
        [jnp.broadcast_to(found[d * groups + g][None], (8, Z)) for g in range(groups)]
        for d in range(3)
    ]

    def solid_velocity(index):
        group = lax.shift_right_logical(index, Z.bit_length() - 1)
        local = index - group * Z
        v = []
        for d in range(3):
            value = jnp.zeros((8, Z), F32)
            for g in range(groups):
                value = jnp.where(group == g, lane_take(tables[d][g], local), value)
            v.append(value)
        return v, 1.0 - 1.5 * (v[0] * v[0] + v[1] * v[1] + v[2] * v[2])

    def halo_copy(vector):
        if vector[2] != 0 and vector[1] != 0:
            row = pl.ds((Y - 1) % 8 if vector[1] == 1 else 0, 1)
            src, dst = zpack.at[side(vector[2]), row], thalo.at[TILE_ID[vector], row]
        elif vector[2] != 0:
            src, dst = zpack.at[side(vector[2])], thalo.at[TILE_ID[vector]]
        elif vector[0] != 0 and vector[1] != 0:
            entry = LEAVING[1, vector[1]].index(LATTICE.index(vector))
            row = pl.ds(X - 1 if vector[0] == 1 else 0, 1)
            src, dst = ypack.at[side(vector[1]), entry, row], thalo.at[TILE_ID[vector], row]
        elif vector[0] != 0:
            src, dst = xpack.at[side(vector[0])], xhalo.at[side(vector[0])]
        else:
            src, dst = ypack.at[side(vector[1])], yhalo.at[side(vector[1])]
        return pltpu.make_async_remote_copy(
            src_ref=src, dst_ref=dst, send_sem=sent.at[0], recv_sem=edges_in.at[0],
            device_id=device(vector), device_id_type=MESH,
        )

    def when_there(vector, action):
        pl.when(exists(vector))(action)

    entry8 = lane8 // chunks
    for sign in (1, -1):
        v, rest = solid_velocity(edge_index[sign])
        along = v[2] if sign == 1 else -v[2]
        base = jnp.zeros((8, Z), F32)
        for entry, i in enumerate(LEAVING[2, sign]):
            here = entry8 == entry
            base = jnp.where(here, F32(WEIGHTS[i]), base)
            for d in range(2):
                c = LATTICE[i][d]
                if c:
                    along = jnp.where(here, along + v[d] if c == 1 else along - v[d], along)
        zpack[side(sign)] = zpack[side(sign)] + edge_share[sign] * base * (
            rest + (4.5 * along + 3.0) * along
        )
    for vector in HALOS[::-1]:
        if vector[2] != 0:
            when_there(vector, lambda vector=vector: halo_copy(vector).start())
    for sign in (1, -1):
        v, rest = solid_velocity(iv[line_of[sign], :])
        share = state[5, line_of[sign], :]
        for entry, i in enumerate(LEAVING[1, sign]):
            along = dot(LATTICE[i], v)
            ypack[side(sign), entry] = ypack[side(sign), entry] + share * F32(WEIGHTS[i]) * (
                rest + (4.5 * along + 3.0) * along
            )
    for vector in HALOS[::-1]:
        if vector[2] == 0 and vector[1] != 0:
            when_there(vector, lambda vector=vector: halo_copy(vector).start())

    def collide_solid(r):
        rows = pl.ds(pl.multiple_of(r * 8, 8), 8)
        v, rest = solid_velocity(iv[rows, :])
        share = state[5, rows, :]
        scaled = {w: w * share for w in sorted(set(WEIGHTS))}
        rel[PLACE[0], rows, :] = rel[PLACE[0], rows, :] + scaled[WEIGHTS[0]] * rest
        for i in range(1, 19, 2):
            j = OPPOSITE[i]
            ps = dot(LATTICE[i], v)
            even = scaled[WEIGHTS[i]] * (rest + 4.5 * ps * ps)
            odd = scaled[WEIGHTS[i]] * (3.0 * ps)
            rel[PLACE[i], rows, :] = rel[PLACE[i], rows, :] + (even + odd)
            rel[PLACE[j], rows, :] = rel[PLACE[j], rows, :] + (even - odd)

    def x_faces(sign):
        face = side(sign)
        for h in range(halves):
            row = ((X - 1) * Y if sign == 1 else 0) + h * 8
            rows = pl.ds(row, 8)
            v, rest = solid_velocity(iv[rows, :])
            share = state[5, rows, :]
            for entry, i in enumerate(LEAVING[0, sign]):
                along = dot(LATTICE[i], v)
                xpack[face, entry, pl.ds(h * 8, 8)] = rel[PLACE[i], rows, :] + share * F32(
                    WEIGHTS[i]
                ) * (rest + (4.5 * along + 3.0) * along)
        when_there((sign, 0, 0), lambda: halo_copy((sign, 0, 0)).start())

    odd = lax.rem(me[0], 2) == 1
    pl.when(odd)(lambda: x_faces(1))
    pl.when(jnp.logical_not(odd))(lambda: x_faces(-1))

    own = [recs[13, d] for d in range(6)]
    contact = [jnp.zeros((1, slots), F32) for _ in range(3)]
    spans = (X / R, Y / R, Z / R)
    for start in range(0, neighbours, 8):
        used = min(8, neighbours - start)
        lines = [cv[n] for n in range(start, start + used)]
        half = used <= 4
        if half:
            lines = (lines + [jnp.full((4 - used, slots), 27 * slots, I32)] * (used < 4)) * 2
        elif used < 8:
            lines.append(jnp.full((8 - used, slots), 27 * slots, I32))
        entries = jnp.concatenate(lines, axis=0)
        entry_block, local = place_of(entries)
        near = [jnp.zeros((8, slots), F32)] * (2 if half else 3)
        for o in blocks:
            hit = entry_block == o
            lines = [wide(o, d) for d in range(3)]
            if half:
                lines = [jnp.where(sub8 < 4, lines[0], lines[1]), lines[2]]
            near = [
                jnp.where(hit, lane_take(line, local), value) for line, value in zip(lines, near)
            ]
        if half:
            near = [near[0], pltpu.roll(near[0], 4, 0), near[1]]
        nine = jnp.zeros(entry_block.shape, I32)
        for step in (9, 18, 27):
            nine = nine + (entry_block >= step).astype(I32)
        inner = entry_block - 9 * nine
        three = (inner >= 3).astype(I32) + (inner >= 6).astype(I32)
        moves = (nine - 1, three - 1, inner - 3 * three - 1)
        apart = [
            jnp.broadcast_to(own[d], (8, slots)) - (near[d] + moves[d].astype(F32) * spans[d])
            for d in range(3)
        ]
        soften = 1.0 + 0.25 * (apart[0] * apart[0] + apart[1] * apart[1] + apart[2] * apart[2])
        valid = entries < 27 * slots
        if half:
            valid = valid & (sub8 < 4)
        strength = CONTACT_GAIN * valid.astype(F32) / (soften * soften)
        for d in range(3):
            contact[d] = contact[d] + jnp.sum(apart[d] * strength, axis=0, keepdims=True)

    wait_rows(force_rows, forces_in)
    terms = [fsend[13]] + [frecv[o] for o in blocks]
    while len(terms) > 1:
        terms = [sum(terms[n + 1 : n + 2], terms[n]) for n in range(0, len(terms), 2)]
    force = terms[0]
    gravity = (0.0, 0.0, GRAVITY_STEP)
    velocity_new, position_new = [], []
    for d in range(3):
        speed = own[3 + d]
        hydro = force[d : d + 1] - force[3:4] * (SPEED_UNIT * speed)
        velocity = speed + FORCE_SCALE * hydro + contact[d] - gravity[d]
        velocity_new.append(velocity)
        position_new.append(own[d] + velocity * (SPEED_UNIT / R))
    record = jnp.concatenate(position_new + velocity_new + [jnp.zeros((2, slots), F32)], axis=0)

    def routed(n, vector):
        origin = jnp.broadcast_to(taken_from[n : n + 1], (8, slots))
        moved = lane_take(record, jnp.where(origin > 0, origin - 1, 0))
        shift = jnp.zeros((8, slots), F32)
        for d in range(3):
            if vector[d]:
                shift = jnp.where(row_id == d, F32(vector[d] * spans[d]), shift)
        return jnp.where(origin > 0, moved - shift, F32(0.0))

    def move_copy(n):
        return pltpu.make_async_remote_copy(
            src_ref=msend.at[n], dst_ref=mrecv.at[n], send_sem=sent.at[0],
            recv_sem=edges_in.at[0], device_id=device(FACES[n]), device_id_type=MESH,
        )

    for n, vector in enumerate(FACES):
        msend[n] = routed(n, vector)
    stay = routed(6, (0, 0, 0))
    for n, vector in reversed(list(enumerate(FACES))):
        when_there(vector, lambda n=n: move_copy(n).start())

    pl.when(odd)(lambda: x_faces(-1))
    pl.when(jnp.logical_not(odd))(lambda: x_faces(1))

    def collide_rest(step, carry):
        for n in range(SOLID_UNROLL):
            collide_solid(step * SOLID_UNROLL + n)
        return carry

    lax.fori_loop(0, chunks // SOLID_UNROLL, collide_rest, 0)

    wait_rows(sent_rows, sent)
    wait_rows(edge_rows, edges_in)
    for n in range(len(FACES)):
        stay = stay + mrecv[n]
    for d in range(6):
        moved[d] = stay[d : d + 1]


def pass_kernel(sizes, shape, rel, xhalo, yhalo, thalo, moved, out_hbm, part_out, pv, out_sem):
    X, Y, Z = shape
    chunks = X * Y // 8
    halves = Y // 8
    me = tuple(lax.axis_index(a) for a in ("gx", "gy", "gz"))
    part_copy = pltpu.make_async_copy(moved, part_out, out_sem.at[1])
    part_copy.start()
    suby = lax.broadcasted_iota(I32, (Y, Z), 0)
    laney = lax.broadcasted_iota(I32, (Y, Z), 1)
    open_back = {
        (axis, sign): (me[axis] > 0) if sign == 1 else (me[axis] < sizes[axis] - 1)
        for axis in range(3)
        for sign in (1, -1)
    }
    target = {1: 0, -1: Z - 1}
    row_edge = {1: 0, -1: Y - 1}

    def edge_mask(c):
        mask = None
        if c[1]:
            blocked = jnp.broadcast_to(jnp.where(open_back[1, c[1]], -1, row_edge[c[1]]), (Y, Z))
            mask = suby != blocked
        if c[2]:
            blocked = jnp.broadcast_to(jnp.where(open_back[2, c[2]], -1, target[c[2]]), (Y, Z))
            other = laney != blocked
            mask = other if mask is None else mask & other
        return mask

    for i in PASS_ORDER:
        c = LATTICE[i]
        j = OPPOSITE[i]
        mask = edge_mask(c)
        for x in range(X):
            from_x = x - c[0]
            inside_x = 0 <= from_x < X
            wrapped = from_x % X
            if inside_x:
                slab = rel[PLACE[i], from_x * Y : (from_x + 1) * Y, :]
            else:
                slab = xhalo[side(c[0]), LEAVING[0, c[0]].index(i)]
            turn = 1 if c[2] == 1 else Z - 1
            if c[2]:
                entry = LEAVING[2, c[2]].index(i)
                tile = thalo[TILE_ID[(0, 0, c[2])]] if inside_x else thalo[TILE_ID[(c[0], 0, c[2])]]
                columns = []
                for h in range(halves):
                    column = entry * chunks + wrapped * halves + h
                    amount = (target[c[2]] - column) % Z
                    columns.append(pltpu.roll(tile, amount, 1) if amount else tile)
                edge_columns = jnp.concatenate(columns, axis=0)
                slab = jnp.where(laney == target[c[2]], edge_columns, pltpu.roll(slab, turn, 1))
            if c[1]:
                entry = LEAVING[1, c[1]].index(i)
                if inside_x:
                    line = yhalo[side(c[1]), entry, from_x : from_x + 1, :]
                else:
                    line = thalo[TILE_ID[(c[0], c[1], 0)], wrapped : wrapped + 1, :]
                if c[2]:
                    entry = LEAVING[2, c[2]].index(i)
                    last = (Y - 1) if c[1] == 1 else 0
                    column = entry * chunks + from_x * halves + last // 8
                    amount = (target[c[2]] - column) % Z
                    tile = thalo[TILE_ID[c]]
                    tile = pltpu.roll(tile, amount, 1) if amount else tile
                    corner = tile[last % 8 : last % 8 + 1]
                    tile = yhalo[side(c[1]), LEAVING[1, c[1]].index(i)]
                    line = pltpu.roll(tile, turn, 1)[from_x : from_x + 1]
                    line = jnp.where(laney[0:1] == target[c[2]], corner, line)
                slab = pltpu.roll(slab, 1 if c[1] == 1 else Y - 1, 0)
                slab = jnp.where(suby == row_edge[c[1]], jnp.broadcast_to(line, (Y, Z)), slab)
            mirror = rel[PLACE[j], x * Y : (x + 1) * Y, :] if c != (0, 0, 0) else None
            if mask is not None:
                slab = jnp.where(mask, slab, mirror)
            if not inside_x:
                closed = jnp.broadcast_to(open_back[0, c[0]].astype(I32), (Y, Z))
                slab = jnp.where(closed > 0, slab, mirror)
            pv[i, x * Y : (x + 1) * Y, :] = slab
        pltpu.make_async_copy(pv.at[i], out_hbm.at[i], out_sem.at[0]).start()

    part_copy.wait()
    pltpu.make_async_copy(pv, out_hbm, out_sem.at[0]).wait()


def body(sizes, populations, solid_fraction, intersection, touch, particles, contacts, dest_code, dest_slot):
    count, X, Y, Z = populations.shape
    slots = particles.shape[4]
    touches = touch.shape[3]
    neighbours = contacts.shape[3]
    any_space = pl.BlockSpec(memory_space=pl.ANY)
    dma = pltpu.SemaphoreType.DMA
    vmem = pl.BlockSpec(memory_space=pltpu.VMEM)
    values = (
        populations.reshape(count, X * Y, Z),
        solid_fraction.reshape(X * Y, Z),
        intersection.reshape(X * Y, Z),
        touch.reshape(1, touches),
        particles.reshape(6, 1, slots),
        contacts.reshape(neighbours, 1, slots),
        dest_code.reshape(1, slots),
        dest_slot.reshape(1, slots),
    )
    handed = pl.pallas_call(
        functools.partial(kernel, sizes, (X, Y, Z)),
        out_shape=(
            pltpu.VMEM((count, X * Y, Z), F32),
            pltpu.VMEM((2, 5, Y, Z), F32),
            pltpu.VMEM((2, 5, X, Z), F32),
            pltpu.VMEM((len(TILES), 8, Z), F32),
            pltpu.VMEM((6, 1, slots), F32),
        ),
        in_specs=[pl.BlockSpec(memory_space=pltpu.HBM)] * 8,
        out_specs=(vmem,) * 5,
        scratch_shapes=[
            pltpu.VMEM((count, X * Y, Z), F32),
            pltpu.VMEM((X * Y, Z), F32),
            pltpu.VMEM((X * Y, Z), I32),
            pltpu.VMEM((1, touches), I32),
            pltpu.VMEM((neighbours, 1, slots), I32),
            pltpu.VMEM((1, slots), I32),
            pltpu.VMEM((1, slots), I32),
            pltpu.VMEM((27, 6, 1, slots), F32),
            pltpu.VMEM((6, X * Y, Z), F32),
            pltpu.VMEM((touches // LO, Z), F32),
            pltpu.VMEM((27, 4, slots), F32),
            pltpu.VMEM((27, 4, slots), F32),
            pltpu.VMEM((2, 5, X, Z), F32),
            pltpu.VMEM((2, 8, Z), F32),
            pltpu.VMEM((len(FACES), 8, slots), F32),
            pltpu.VMEM((len(FACES), 8, slots), F32),
            pltpu.VMEM((slots, 2 * touches), BF16),
            pltpu.VMEM((26 * 10 + 10 * (X + Y) + 8 * (len(TILES) + len(FACES)), Z), F32),
            pltpu.VMEM((2, 5, Y, Z), F32),
            dma((2 + X * Y // (8 * SUM_UNROLL),)),
            dma((1,)),
            dma((1,)),
            dma((1,)),
            dma((1,)),
            pltpu.SemaphoreType.REGULAR((1,)),
        ],
        compiler_params=pltpu.CompilerParams(
            collective_id=0, has_side_effects=True, vmem_limit_bytes=GRANT
        ),
    )(*[pltpu.with_memory_space_constraint(value, pltpu.HBM) for value in values])
    out, moved = pl.pallas_call(
        functools.partial(pass_kernel, sizes, (X, Y, Z)),
        out_shape=(
            jax.ShapeDtypeStruct((count, X * Y, Z), F32),
            jax.ShapeDtypeStruct((6, 1, slots), F32),
        ),
        in_specs=[vmem] * 5,
        out_specs=(any_space, any_space),
        scratch_shapes=[pltpu.VMEM((count, X * Y, Z), F32), dma((2,))],
        compiler_params=pltpu.CompilerParams(vmem_limit_bytes=GRANT),
    )(*[pltpu.with_memory_space_constraint(value, pltpu.VMEM) for value in handed])
    return (out.reshape(count, X, Y, Z), moved.reshape(1, 1, 1, 6, slots))


def solution(mesh):
    placed = (
        P(None, "gx", "gy", "gz"),
        P("gx", "gy", "gz"),
        P("gx", "gy", "gz"),
        P("gx", "gy", "gz", None),
        P("gx", "gy", "gz", None, None),
        P("gx", "gy", "gz", None, None),
        P("gx", "gy", "gz", None),
        P("gx", "gy", "gz", None),
    )
    sizes = tuple(mesh.shape[axis] for axis in ("gx", "gy", "gz"))
    return jax.shard_map(
        functools.partial(body, sizes),
        mesh=mesh,
        in_specs=placed,
        out_specs=(P(None, "gx", "gy", "gz"), P("gx", "gy", "gz", None, None)),
        check_vma=False,
    )
```

```python
import functools
import itertools

import jax
import jax.numpy as jnp
from jax import lax
from jax.experimental import pallas as pl
from jax.experimental.pallas import tpu as pltpu
from jax.sharding import PartitionSpec as P

R = 8

LATTICE = [
    (0, 0, 0),
    (1, 0, 0),
    (-1, 0, 0),
    (0, 1, 0),
    (0, -1, 0),
    (0, 0, 1),
    (0, 0, -1),
    (1, 1, 0),
    (-1, -1, 0),
    (1, -1, 0),
    (-1, 1, 0),
    (1, 0, 1),
    (-1, 0, -1),
    (1, 0, -1),
    (-1, 0, 1),
    (0, 1, 1),
    (0, -1, -1),
    (0, 1, -1),
    (0, -1, 1),
]
OPPOSITE = [0, 2, 1, 4, 3, 6, 5, 8, 7, 10, 9, 12, 11, 14, 13, 16, 15, 18, 17]
WEIGHTS = [1.0 / 3.0] + [1.0 / 18.0] * 6 + [1.0 / 36.0] * 12
RELAX_TIME = 0.8
SPEED_UNIT = 0.05
FORCE_SCALE = 0.1
CONTACT_GAIN = 1.0
GRAVITY_STEP = 0.1

MESH = pl.DeviceIdType.MESH
F32 = jnp.float32
BF16 = jnp.bfloat16
I32 = jnp.int32

LEAVING = {
    (axis, sign): [i for i, c in enumerate(LATTICE) if c[axis] == sign]
    for axis in range(3)
    for sign in (1, -1)
}
ORDER = LEAVING[0, 1] + LEAVING[0, -1] + [i for i, c in enumerate(LATTICE) if c[0] == 0]
PLACE = {i: n for n, i in enumerate(ORDER)}
HALOS = [c for c in LATTICE if c != (0, 0, 0)]
HALO_ID = {c: n for n, c in enumerate(HALOS)}
PASS_ORDER = sorted(range(19), key=lambda i: (LATTICE[i][2] != 0, i))
TILES = [c for c in HALOS if c[2] != 0] + [c for c in HALOS if c[2] == 0 and c[0] != 0 and c[1] != 0]
TILE_ID = {c: n for n, c in enumerate(TILES)}
FACES = [(1, 0, 0), (-1, 0, 0), (0, 1, 0), (0, -1, 0), (0, 0, 1), (0, 0, -1)]
LO = 8
GRANT = 16 * 2**20
SUM_UNROLL = 8
EARLY_STEPS = 1
COLLIDE_UNROLL = 2
SOLID_UNROLL = 8
BEYOND = (1, 1, 1)
BEFORE = (-1, -1, -1)


def block_id(vector):
    return 9 * (vector[0] + 1) + 3 * (vector[1] + 1) + vector[2] + 1


def side(sign):
    return 0 if sign == 1 else 1


def lane_take(table, index):
    return jnp.take_along_axis(table, index, axis=1, mode="promise_in_bounds")


def nt_dot(left, right):
    return lax.dot_general(left, right, (((1,), (1,)), ((), ())), preferred_element_type=F32)


def split_pair(value):
    high = value.astype(BF16).astype(F32)
    return high, value - high


def kernel(
    sizes,
    shape,
    pops_hbm, frac_hbm, inter_hbm, touch_hbm, part_hbm, cont_hbm, code_hbm, slot_hbm,
    rel, xhalo, yhalo, thalo, moved,
    pv, fv, iv, tv, cv, codev, slotv,
    recs, state, sums, fsend, frecv, ypack, zpack, msend, mrecv,
    picked, ruler, xpack, in_sem, sent, recs_in, forces_in, edges_in, ready,
):
    X, Y, Z = shape
    slots = recs.shape[3]
    touches = tv.shape[1]
    neighbours = cv.shape[0]
    chunks = X * Y // 8
    halves = Y // 8
    me = tuple(lax.axis_index(a) for a in ("gx", "gy", "gz"))

    cell_ins = [
        pltpu.make_async_copy(inter_hbm, iv, in_sem.at[1]),
        pltpu.make_async_copy(frac_hbm, fv, in_sem.at[1]),
    ]
    small_ins = [
        pltpu.make_async_copy(src, dst, in_sem.at[0])
        for src, dst in [
            (part_hbm, recs.at[13]), (touch_hbm, tv), (cont_hbm, cv), (code_hbm, codev),
            (slot_hbm, slotv),
        ]
    ]
    small_rows = (touches + (neighbours + 8) * slots) // Z
    cells_done = pltpu.make_async_copy(pops_hbm.at[0:2], pv.at[0:2], in_sem.at[1])
    small_done = pltpu.make_async_copy(
        pops_hbm.at[0, 0:small_rows], pv.at[0, 0:small_rows], in_sem.at[0]
    )
    steps = chunks // SUM_UNROLL
    span = SUM_UNROLL * 8

    def pops_in(step):
        rows = pl.ds(pl.multiple_of(step * span, span), span)
        return pltpu.make_async_copy(pops_hbm.at[:, rows], pv.at[:, rows], in_sem.at[2 + step])

    there = {
        (axis, sign): (me[axis] < sizes[axis] - 1) if sign == 1 else (me[axis] > 0)
        for axis in range(3)
        for sign in (1, -1)
    }

    def exists(vector):
        flags = [there[axis, step] for axis, step in enumerate(vector) if step]
        return functools.reduce(lambda p, q: p & q, flags)

    def device(vector):
        return tuple(position + step for position, step in zip(me, vector))

    def steps_along(axis):
        if sizes[axis] == 1:
            return [((0,), None)]
        if sizes[axis] == 2:
            return [((0, 1 - 2 * me[axis]), None)]
        return [((-1,), there[axis, -1]), ((0,), None), ((1,), there[axis, 1])]

    def far(vector):
        return sum(1 for step in vector if not (isinstance(step, int) and step == 0))

    def each_neighbour(action, skip=(2, 2, 2), allow={}, levels=(-1, 0, 1)):
        groups = []
        for choice in itertools.product(*[steps_along(axis) for axis in range(3)]):
            level = choice[2][0][0]
            if sizes[2] > 2 and level not in levels:
                continue
            flags = [flag for _, flag in choice if flag is not None]
            if level in allow:
                flags.append(allow[level])
            vectors = list(itertools.product(*[values for values, _ in choice]))
            groups.append((flags, sorted([v for v in vectors if far(v)], key=far, reverse=True)))

        def act(vectors):
            for vector in vectors:
                do = functools.partial(action, block_id(vector), vector)
                pairs = list(zip(range(3), vector, skip))
                fixed = [p for p in pairs if isinstance(p[1], int)]
                moving = [p for p in pairs if not isinstance(p[1], int)]
                if any(step != other for _, step, other in fixed) or 2 in skip:
                    do()
                elif moving and all(other for _, _, other in moving):
                    apart = [jnp.logical_not(there[axis, other]) for axis, _, other in moving]
                    pl.when(functools.reduce(lambda p, q: p | q, apart))(do)
                elif moving:
                    do()

        for flags, vectors in sorted(groups, key=lambda g: max(map(far, g[1]), default=0), reverse=True):
            run = functools.partial(act, vectors)
            if flags:
                pl.when(functools.reduce(lambda p, q: p & q, flags))(run)
            else:
                run()

    windows = [
        [0] if size == 1 else [0 - at, 1 - at] if size == 2 else [-1, 0, 1]
        for size, at in zip(sizes, me)
    ]
    blocks = [block_id((x, y, z)) for x in windows[0] for y in windows[1] for z in windows[2]]

    barrier = pltpu.get_barrier_semaphore()

    half = sizes[2] // 2
    split = sizes[2] > 2
    alone_up = there[2, 1] & (me[2] >= half)
    alone_down = me[2] > half
    not_up = {1: jnp.logical_not(alone_up)} if split else {}
    not_down = {-1: jnp.logical_not(alone_down)} if split else {}

    def greet(o, vector):
        pl.semaphore_signal(barrier, inc=1, device_id=device(vector), device_id_type=MESH)

    pops_in(0).start()
    for copy in small_ins + cell_ins:
        copy.start()
    for step in range(1, steps):
        pops_in(step).start()
    each_neighbour(greet, BEFORE, not_down)

    around = [
        (me[axis] > 0).astype(I32) + (me[axis] < sizes[axis] - 1).astype(I32) for axis in range(3)
    ]
    options = [[0] if size == 1 else [1] if size == 2 else [1, 2] for size in sizes]
    nearby = lambda n: (n[0] + 1) * (n[1] + 1) * (n[2] + 1) - 1
    record_rows = lambda n: 6 * nearby(n)
    force_rows = lambda n: 4 * nearby(n)

    def edge_rows(n):
        x, y, z = n
        tiles = 8 * (z + x * z + x + y + z) + x * y + y * z
        return 5 * (Y * x + X * y) + tiles

    sent_rows = lambda n: record_rows(n) + force_rows(n) + edge_rows(n)

    plane = (around[0] + 1) * (around[1] + 1)
    waiting = exists(BEYOND).astype(I32)
    if split:
        waiting = jnp.where(alone_up, plane, waiting)
    count = nearby(around) - waiting

    def wait_rows(measure, semaphore):
        amount = measure(around)
        for rows in sorted({measure(n) for n in itertools.product(*options)}):
            if rows:
                part = ruler.at[0:rows]
                copy = pltpu.make_async_copy(part, part, semaphore.at[0])
                pl.when(amount == rows)(copy.wait)

    def record_copy(o, vector):
        return pltpu.make_async_remote_copy(
            src_ref=recs.at[13], dst_ref=recs.at[26 - o], send_sem=sent.at[0],
            recv_sem=recs_in.at[0], device_id=device(vector), device_id_type=MESH,
        )

    sub8 = lax.broadcasted_iota(I32, (8, Z), 0)
    lane8 = lax.broadcasted_iota(I32, (8, Z), 1)
    high_count = touches // LO
    sub_high = lax.broadcasted_iota(I32, (high_count, Z), 0)

    def gather_pieces(r):
        rows = pl.ds(pl.multiple_of(r * 8, 8), 8)
        f = [pv[i, rows, :] for i in range(19)]
        rho = functools.reduce(lambda a, b: a + b, f)
        momentum = []
        for axis in range(3):
            terms = None
            for i in LEAVING[axis, 1]:
                diff = f[i] - f[OPPOSITE[i]]
                terms = diff if terms is None else terms + diff
            momentum.append(terms)
        index = iv[rows, :]
        eps = fv[rows, :]
        weight = jnp.where(
            index < touches,
            eps * (RELAX_TIME - 0.5) / (1.0 - eps + (RELAX_TIME - 0.5)),
            F32(0.0),
        )
        inverse = 1.0 / rho
        state[0, rows, :] = rho
        for axis in range(3):
            state[1 + axis, rows, :] = momentum[axis] * inverse
        state[4, rows, :] = weight
        wanted = [weight * m for m in momentum] + [weight * rho]
        state[5, rows, :] = wanted[3]
        pairs = [split_pair(w) for w in wanted]
        pieces = [p[0] for p in pairs] + [p[1] for p in pairs]
        high = index // LO if LO & (LO - 1) else lax.shift_right_logical(index, LO.bit_length() - 1)
        low = index - high * LO
        return pieces, high, low

    def gather_pairs(pieces, high, low):
        left, right = [], []
        for row in range(8):
            high_row = jnp.broadcast_to(high[row : row + 1], (high_count, Z))
            match = jnp.broadcast_to(low[row : row + 1], (8, Z)) == sub8
            left.append(jnp.where(high_row == sub_high, F32(1.0), F32(0.0)).astype(BF16))
            right.append(
                jnp.concatenate(
                    [
                        jnp.where(match, jnp.broadcast_to(pieces[p][row : row + 1], (8, Z)), F32(0.0))
                        for p in range(8)
                    ],
                    axis=0,
                ).astype(BF16)
            )
        return right, left

    def gather_sums(step, total):
        pops_in(step).wait()
        right, left = [], []
        for n in range(SUM_UNROLL):
            more_right, more_left = gather_pairs(*gather_pieces(step * SUM_UNROLL + n))
            right += more_right
            left += more_left
        return total + nt_dot(jnp.concatenate(left, axis=1), jnp.concatenate(right, axis=1))

    groups = touches // Z

    def spread_sums(total):
        sums[:, 0 : 8 * LO] = total
        both = sums[...]
        lane_high = lax.shift_right_logical(lane8, LO.bit_length() - 1)
        lane_low = lane8 - lane_high * LO
        parts = []
        for g in range(groups):
            lines = []
            for q in range(4):
                line = jnp.zeros((8, Z), F32)
                for part in range(Z // (8 * LO)):
                    first_row = g * (Z // LO) + part * 8
                    rows = both[first_row : first_row + 8]
                    taken = lane_take(rows, q * LO + lane_low)
                    taken = taken + lane_take(rows, (4 + q) * LO + lane_low)
                    line = line + jnp.where(sub8 + part * 8 == lane_high, taken, F32(0.0))
                lines.append(jnp.sum(line, axis=0, keepdims=True))
            quad = jnp.concatenate(lines, axis=0)
            first, second = split_pair(quad)
            parts.append((first, second))
        tables = [
            jnp.concatenate([jnp.concatenate([part[h]] * 2, axis=0) for part in parts], axis=1)
            for h in range(2)
        ]
        block8 = jnp.broadcast_to(touch_block, (8, touches))
        upper = lax.broadcasted_iota(I32, (8, touches), 0) < 4
        lefts = []
        for n in range(0, len(blocks), 2):
            hit = block8 == jnp.where(upper, blocks[n], blocks[min(n + 1, len(blocks) - 1)])
            lefts.append(
                jnp.concatenate([jnp.where(hit, table, F32(0.0)) for table in tables], axis=1)
            )
        spread = nt_dot(jnp.concatenate(lefts, axis=0).astype(BF16), picked[...])
        for n, o in enumerate(blocks):
            fsend[o] = spread[4 * n : 4 * n + 4]

    middle = (lax.rem(me[0], 2) == 1) & there[0, 1]
    idle = (there[1, 1] & there[2, 1]) | (middle & (there[1, 1] | there[2, 1]))
    if split:
        idle = jnp.where(me[2] < half, idle, middle & there[1, 1])
    first_steps = jnp.where(idle, steps, EARLY_STEPS)
    if split:
        last_y = jnp.logical_not(there[1, 1])
        top = jnp.logical_not(there[2, 1])
        first_steps = jnp.where((me[2] >= half) & (last_y | top), 0, first_steps)
        first_steps = jnp.where((me[2] >= half) & middle, jnp.where(last_y, 1, steps), first_steps)
    sums[...] = jnp.zeros(sums.shape, F32)
    frecv[13] = jnp.zeros(frecv.shape[1:], F32)

    def clear(ids):
        for o in ids:
            recs[o] = jnp.zeros(recs.shape[1:], F32)
            frecv[o] = jnp.zeros(frecv.shape[1:], F32)

    for choice in itertools.product(*[steps_along(axis) for axis in range(3)]):
        flags = [flag for _, flag in choice if flag is not None]
        if flags:
            ids = [block_id(vector) for vector in itertools.product(*[values for values, _ in choice])]
            present = functools.reduce(lambda p, q: p & q, flags)
            pl.when(jnp.logical_not(present))(functools.partial(clear, ids))
    for n, vector in enumerate(FACES):
        back = tuple(-step for step in vector)

        def clear_moved(n=n):
            mrecv[n] = jnp.zeros(mrecv.shape[1:], F32)

        pl.when(jnp.logical_not(exists(back)))(clear_moved)

    small_done.wait()
    touch_row = tv[...]
    touch_block = lax.shift_right_logical(touch_row, slots.bit_length() - 1)
    touch_slot = touch_row - touch_block * slots
    chosen = jnp.where(
        jnp.broadcast_to(touch_slot, (slots, touches))
        == lax.broadcasted_iota(I32, (slots, touches), 0),
        F32(1.0),
        F32(0.0),
    ).astype(BF16)
    picked[:, 0:touches] = chosen
    picked[:, touches : 2 * touches] = chosen

    pl.when(first_steps > 0)(cells_done.wait)
    total = lax.fori_loop(0, first_steps, gather_sums, jnp.zeros((high_count, 8 * LO), F32))
    pl.when(idle)(lambda: spread_sums(total))

    pl.semaphore_wait(barrier, count)
    def answer(o, vector):
        pl.semaphore_signal(ready.at[0], inc=1, device_id=device(vector), device_id_type=MESH)

    answer_far = functools.partial(answer, block_id(BEFORE), BEFORE)
    if split:
        pl.when(alone_down)(lambda: each_neighbour(answer, levels=(-1,)))
        pl.when(exists(BEFORE) & jnp.logical_not(alone_down))(answer_far)
    else:
        pl.when(exists(BEFORE))(answer_far)
    each_neighbour(lambda o, v: record_copy(o, v).start(), BEYOND, not_up)

    pl.when(first_steps == 0)(cells_done.wait)
    total = lax.fori_loop(first_steps, steps, gather_sums, total)
    pl.when(jnp.logical_not(idle))(lambda: spread_sums(total))

    def force_copy(o, vector):
        return pltpu.make_async_remote_copy(
            src_ref=fsend.at[o], dst_ref=frecv.at[26 - o], send_sem=sent.at[0],
            recv_sem=forces_in.at[0], device_id=device(vector), device_id_type=MESH,
        )

    each_neighbour(lambda o, v: force_copy(o, v).start(), BEYOND, not_up)

    code = codev[...]
    wanted_codes = [9 * (v[0] + 1) + 3 * (v[1] + 1) + v[2] + 1 for v in FACES] + [13]
    slot_id = lax.broadcasted_iota(I32, (8, slots), 1).astype(F32) + 1.0
    code_of = jnp.full((8, slots), 27, I32)
    row_id = lax.broadcasted_iota(I32, (8, slots), 0)
    for n, c in enumerate(wanted_codes):
        code_of = jnp.where(row_id == n, c, code_of)
    route = jnp.where(jnp.broadcast_to(code, (8, slots)) == code_of, slot_id, F32(0.0)).astype(BF16)
    place = jnp.where(
        jnp.broadcast_to(slotv[...], (slots, slots)) == lax.broadcasted_iota(I32, (slots, slots), 0),
        F32(1.0),
        F32(0.0),
    ).astype(BF16)
    taken_from = nt_dot(route, place).astype(I32)

    def dot(c, vec):
        value = None
        for axis in range(3):
            if c[axis]:
                term = vec[axis] if c[axis] == 1 else -vec[axis]
                value = term if value is None else value + term
        return value

    def collide_fluid(r):
        rows = pl.ds(pl.multiple_of(r * 8, 8), 8)
        rho = state[0, rows, :]
        u = [state[1 + d, rows, :] for d in range(3)]
        weight = state[4, rows, :]
        keep = (1.0 - weight) * (1.0 / RELAX_TIME)
        rest_u = 1.0 - 1.5 * (u[0] * u[0] + u[1] * u[1] + u[2] * u[2])
        scaled = {w: w * rho for w in sorted(set(WEIGHTS))}
        f0 = pv[0, rows, :]
        eq_u = scaled[WEIGHTS[0]] * rest_u
        rel[PLACE[0], rows, :] = f0 - keep * (f0 - eq_u) - weight * eq_u
        for i in range(1, 19, 2):
            j = OPPOSITE[i]
            share = scaled[WEIGHTS[i]]
            pu = dot(LATTICE[i], u)
            even = share * (rest_u + 4.5 * pu * pu)
            odd = share * (3.0 * pu)
            fi, fj = pv[i, rows, :], pv[j, rows, :]
            ui, uj = even + odd, even - odd
            diff = fj - fi
            rel[PLACE[i], rows, :] = fi - keep * (fi - ui) + weight * (diff - uj)
            rel[PLACE[j], rows, :] = fj - keep * (fj - uj) - weight * (diff + ui)

    def collide_some(step, carry):
        for n in range(COLLIDE_UNROLL):
            collide_fluid(step * COLLIDE_UNROLL + n)
        return carry

    lax.fori_loop(0, chunks // COLLIDE_UNROLL, collide_some, 0)

    edges = {(axis, sign): n for n, (axis, sign) in enumerate([(1, 1), (1, -1), (2, 1), (2, -1)])}
    edge_index, edge_share, line_of = {}, {}, {}
    for sign in (1, -1):
        line = pl.ds(Y - 1 if sign == 1 else 0, X, stride=Y)
        for entry, i in enumerate(LEAVING[1, sign]):
            ypack[side(sign), entry] = rel[PLACE[i], line, :]
        line_of[sign] = line

    def pack_columns(read, entries, edge, start):
        packed = start
        for entry in range(entries):
            for r in range(chunks):
                column = entry * chunks + r
                turned = read(entry, pl.ds(r * 8, 8))
                if (column - edge) % Z:
                    turned = pltpu.roll(turned, (column - edge) % Z, 1)
                packed = jnp.where(lane8 == column, turned, packed)
        return packed

    repeat = lax.rem(lane8, chunks)
    for sign in (1, -1):
        edge = Z - 1 if sign == 1 else 0
        leaving = LEAVING[2, sign]
        zpack[side(sign)] = pack_columns(
            lambda entry, rows: rel[PLACE[leaving[entry]], rows, :], 5, edge, jnp.zeros((8, Z), F32)
        )
        share = pack_columns(lambda entry, rows: state[5, rows, :], 1, edge, jnp.zeros((8, Z), F32))
        index = pack_columns(
            lambda entry, rows: iv[rows, :], 1, edge, jnp.full((8, Z), touches, I32)
        )
        edge_share[sign] = lane_take(share, repeat)
        edge_index[sign] = lane_take(index, repeat)

    def reach_far():
        pl.semaphore_wait(ready.at[0], 1)
        record_copy(block_id(BEYOND), BEYOND).start()
        force_copy(block_id(BEYOND), BEYOND).start()

    def reach_up():
        pl.semaphore_wait(ready.at[0], plane)
        each_neighbour(lambda o, v: record_copy(o, v).start(), levels=(1,))
        each_neighbour(lambda o, v: force_copy(o, v).start(), levels=(1,))

    if split:
        pl.when(alone_up)(reach_up)
        pl.when(exists(BEYOND) & jnp.logical_not(alone_up))(reach_far)
    else:
        pl.when(exists(BEYOND))(reach_far)
    wait_rows(record_rows, recs_in)

    def place_of(index):
        block = lax.shift_right_logical(index, slots.bit_length() - 1)
        return block, index - block * slots

    def wide(o, row):
        return jnp.broadcast_to(recs[o, row], (8, Z))

    index_rows = [touch_row[:, g * Z : (g + 1) * Z] for g in range(groups)]
    unused = [jnp.full((8 - 3 * groups, Z), 27 * slots, I32)] if groups * 3 < 8 else []
    touch_blocks, touch_local = place_of(jnp.concatenate(index_rows * 3 + unused, axis=0))
    found = jnp.zeros((8, Z), F32)
    for o in blocks:
        rows = jnp.where(sub8 < groups, wide(o, 3), jnp.where(sub8 < 2 * groups, wide(o, 4), wide(o, 5)))
        found = jnp.where(touch_blocks == o, lane_take(rows, touch_local), found)
    found = SPEED_UNIT * found
    tables = [
        [jnp.broadcast_to(found[d * groups + g][None], (8, Z)) for g in range(groups)]
        for d in range(3)
    ]

    def solid_velocity(index):
        group = lax.shift_right_logical(index, Z.bit_length() - 1)
        local = index - group * Z
        v = []
        for d in range(3):
            value = jnp.zeros((8, Z), F32)
            for g in range(groups):
                value = jnp.where(group == g, lane_take(tables[d][g], local), value)
            v.append(value)
        return v, 1.0 - 1.5 * (v[0] * v[0] + v[1] * v[1] + v[2] * v[2])

    def halo_copy(vector):
        if vector[2] != 0 and vector[1] != 0:
            row = pl.ds((Y - 1) % 8 if vector[1] == 1 else 0, 1)
            src, dst = zpack.at[side(vector[2]), row], thalo.at[TILE_ID[vector], row]
        elif vector[2] != 0:
            src, dst = zpack.at[side(vector[2])], thalo.at[TILE_ID[vector]]
        elif vector[0] != 0 and vector[1] != 0:
            entry = LEAVING[1, vector[1]].index(LATTICE.index(vector))
            row = pl.ds(X - 1 if vector[0] == 1 else 0, 1)
            src, dst = ypack.at[side(vector[1]), entry, row], thalo.at[TILE_ID[vector], row]
        elif vector[0] != 0:
            src, dst = xpack.at[side(vector[0])], xhalo.at[side(vector[0])]
        else:
            src, dst = ypack.at[side(vector[1])], yhalo.at[side(vector[1])]
        return pltpu.make_async_remote_copy(
            src_ref=src, dst_ref=dst, send_sem=sent.at[0], recv_sem=edges_in.at[0],
            device_id=device(vector), device_id_type=MESH,
        )

    def when_there(vector, action):
        pl.when(exists(vector))(action)

    entry8 = lane8 // chunks
    for sign in (1, -1):
        v, rest = solid_velocity(edge_index[sign])
        along = v[2] if sign == 1 else -v[2]
        base = jnp.zeros((8, Z), F32)
        for entry, i in enumerate(LEAVING[2, sign]):
            here = entry8 == entry
            base = jnp.where(here, F32(WEIGHTS[i]), base)
            for d in range(2):
                c = LATTICE[i][d]
                if c:
                    along = jnp.where(here, along + v[d] if c == 1 else along - v[d], along)
        zpack[side(sign)] = zpack[side(sign)] + edge_share[sign] * base * (
            rest + (4.5 * along + 3.0) * along
        )
    for vector in HALOS[::-1]:
        if vector[2] != 0:
            when_there(vector, lambda vector=vector: halo_copy(vector).start())
    for sign in (1, -1):
        v, rest = solid_velocity(iv[line_of[sign], :])
        share = state[5, line_of[sign], :]
        for entry, i in enumerate(LEAVING[1, sign]):
            along = dot(LATTICE[i], v)
            ypack[side(sign), entry] = ypack[side(sign), entry] + share * F32(WEIGHTS[i]) * (
                rest + (4.5 * along + 3.0) * along
            )
    for vector in HALOS[::-1]:
        if vector[2] == 0 and vector[1] != 0:
            when_there(vector, lambda vector=vector: halo_copy(vector).start())

    def collide_solid(r):
        rows = pl.ds(pl.multiple_of(r * 8, 8), 8)
        v, rest = solid_velocity(iv[rows, :])
        share = state[5, rows, :]
        scaled = {w: w * share for w in sorted(set(WEIGHTS))}
        rel[PLACE[0], rows, :] = rel[PLACE[0], rows, :] + scaled[WEIGHTS[0]] * rest
        for i in range(1, 19, 2):
            j = OPPOSITE[i]
            ps = dot(LATTICE[i], v)
            even = scaled[WEIGHTS[i]] * (rest + 4.5 * ps * ps)
            odd = scaled[WEIGHTS[i]] * (3.0 * ps)
            rel[PLACE[i], rows, :] = rel[PLACE[i], rows, :] + (even + odd)
            rel[PLACE[j], rows, :] = rel[PLACE[j], rows, :] + (even - odd)

    def x_faces(sign):
        face = side(sign)
        for h in range(halves):
            row = ((X - 1) * Y if sign == 1 else 0) + h * 8
            rows = pl.ds(row, 8)
            v, rest = solid_velocity(iv[rows, :])
            share = state[5, rows, :]
            for entry, i in enumerate(LEAVING[0, sign]):
                along = dot(LATTICE[i], v)
                xpack[face, entry, pl.ds(h * 8, 8)] = rel[PLACE[i], rows, :] + share * F32(
                    WEIGHTS[i]
                ) * (rest + (4.5 * along + 3.0) * along)
        when_there((sign, 0, 0), lambda: halo_copy((sign, 0, 0)).start())

    odd = lax.rem(me[0], 2) == 1
    pl.when(odd)(lambda: x_faces(1))
    pl.when(jnp.logical_not(odd))(lambda: x_faces(-1))

    own = [recs[13, d] for d in range(6)]
    contact = [jnp.zeros((1, slots), F32) for _ in range(3)]
    spans = (X / R, Y / R, Z / R)
    for start in range(0, neighbours, 8):
        used = min(8, neighbours - start)
        lines = [cv[n] for n in range(start, start + used)]
        half = used <= 4
        if half:
            lines = (lines + [jnp.full((4 - used, slots), 27 * slots, I32)] * (used < 4)) * 2
        elif used < 8:
            lines.append(jnp.full((8 - used, slots), 27 * slots, I32))
        entries = jnp.concatenate(lines, axis=0)
        entry_block, local = place_of(entries)
        near = [jnp.zeros((8, slots), F32)] * (2 if half else 3)
        for o in blocks:
            hit = entry_block == o
            lines = [wide(o, d) for d in range(3)]
            if half:
                lines = [jnp.where(sub8 < 4, lines[0], lines[1]), lines[2]]
            near = [
                jnp.where(hit, lane_take(line, local), value) for line, value in zip(lines, near)
            ]
        if half:
            near = [near[0], pltpu.roll(near[0], 4, 0), near[1]]
        nine = jnp.zeros(entry_block.shape, I32)
        for step in (9, 18, 27):
            nine = nine + (entry_block >= step).astype(I32)
        inner = entry_block - 9 * nine
        three = (inner >= 3).astype(I32) + (inner >= 6).astype(I32)
        moves = (nine - 1, three - 1, inner - 3 * three - 1)
        apart = [
            jnp.broadcast_to(own[d], (8, slots)) - (near[d] + moves[d].astype(F32) * spans[d])
            for d in range(3)
        ]
        soften = 1.0 + 0.25 * (apart[0] * apart[0] + apart[1] * apart[1] + apart[2] * apart[2])
        valid = entries < 27 * slots
        if half:
            valid = valid & (sub8 < 4)
        strength = CONTACT_GAIN * valid.astype(F32) / (soften * soften)
        for d in range(3):
            contact[d] = contact[d] + jnp.sum(apart[d] * strength, axis=0, keepdims=True)

    wait_rows(force_rows, forces_in)
    terms = [fsend[13]] + [frecv[o] for o in blocks]
    while len(terms) > 1:
        terms = [sum(terms[n + 1 : n + 2], terms[n]) for n in range(0, len(terms), 2)]
    force = terms[0]
    gravity = (0.0, 0.0, GRAVITY_STEP)
    velocity_new, position_new = [], []
    for d in range(3):
        speed = own[3 + d]
        hydro = force[d : d + 1] - force[3:4] * (SPEED_UNIT * speed)
        velocity = speed + FORCE_SCALE * hydro + contact[d] - gravity[d]
        velocity_new.append(velocity)
        position_new.append(own[d] + velocity * (SPEED_UNIT / R))
    record = jnp.concatenate(position_new + velocity_new + [jnp.zeros((2, slots), F32)], axis=0)

    def routed(n, vector):
        origin = jnp.broadcast_to(taken_from[n : n + 1], (8, slots))
        moved = lane_take(record, jnp.where(origin > 0, origin - 1, 0))
        shift = jnp.zeros((8, slots), F32)
        for d in range(3):
            if vector[d]:
                shift = jnp.where(row_id == d, F32(vector[d] * spans[d]), shift)
        return jnp.where(origin > 0, moved - shift, F32(0.0))

    def move_copy(n):
        return pltpu.make_async_remote_copy(
            src_ref=msend.at[n], dst_ref=mrecv.at[n], send_sem=sent.at[0],
            recv_sem=edges_in.at[0], device_id=device(FACES[n]), device_id_type=MESH,
        )

    for n, vector in enumerate(FACES):
        msend[n] = routed(n, vector)
    stay = routed(6, (0, 0, 0))
    for n, vector in reversed(list(enumerate(FACES))):
        when_there(vector, lambda n=n: move_copy(n).start())

    pl.when(odd)(lambda: x_faces(-1))
    pl.when(jnp.logical_not(odd))(lambda: x_faces(1))

    def collide_rest(step, carry):
        for n in range(SOLID_UNROLL):
            collide_solid(step * SOLID_UNROLL + n)
        return carry

    lax.fori_loop(0, chunks // SOLID_UNROLL, collide_rest, 0)

    wait_rows(sent_rows, sent)
    wait_rows(edge_rows, edges_in)
    for n in range(len(FACES)):
        stay = stay + mrecv[n]
    for d in range(6):
        moved[d] = stay[d : d + 1]


def pass_kernel(sizes, shape, rel, xhalo, yhalo, thalo, moved, out_hbm, part_out, pv, out_sem):
    X, Y, Z = shape
    chunks = X * Y // 8
    halves = Y // 8
    me = tuple(lax.axis_index(a) for a in ("gx", "gy", "gz"))
    part_copy = pltpu.make_async_copy(moved, part_out, out_sem.at[1])
    part_copy.start()
    suby = lax.broadcasted_iota(I32, (Y, Z), 0)
    laney = lax.broadcasted_iota(I32, (Y, Z), 1)
    open_back = {
        (axis, sign): (me[axis] > 0) if sign == 1 else (me[axis] < sizes[axis] - 1)
        for axis in range(3)
        for sign in (1, -1)
    }
    target = {1: 0, -1: Z - 1}
    row_edge = {1: 0, -1: Y - 1}

    def edge_mask(c):
        mask = None
        if c[1]:
            blocked = jnp.broadcast_to(jnp.where(open_back[1, c[1]], -1, row_edge[c[1]]), (Y, Z))
            mask = suby != blocked
        if c[2]:
            blocked = jnp.broadcast_to(jnp.where(open_back[2, c[2]], -1, target[c[2]]), (Y, Z))
            other = laney != blocked
            mask = other if mask is None else mask & other
        return mask

    for i in PASS_ORDER:
        c = LATTICE[i]
        j = OPPOSITE[i]
        mask = edge_mask(c)
        for x in range(X):
            from_x = x - c[0]
            inside_x = 0 <= from_x < X
            wrapped = from_x % X
            if inside_x:
                slab = rel[PLACE[i], from_x * Y : (from_x + 1) * Y, :]
            else:
                slab = xhalo[side(c[0]), LEAVING[0, c[0]].index(i)]
            turn = 1 if c[2] == 1 else Z - 1
            if c[2]:
                entry = LEAVING[2, c[2]].index(i)
                tile = thalo[TILE_ID[(0, 0, c[2])]] if inside_x else thalo[TILE_ID[(c[0], 0, c[2])]]
                columns = []
                for h in range(halves):
                    column = entry * chunks + wrapped * halves + h
                    amount = (target[c[2]] - column) % Z
                    columns.append(pltpu.roll(tile, amount, 1) if amount else tile)
                edge_columns = jnp.concatenate(columns, axis=0)
                slab = jnp.where(laney == target[c[2]], edge_columns, pltpu.roll(slab, turn, 1))
            if c[1]:
                entry = LEAVING[1, c[1]].index(i)
                if inside_x:
                    line = yhalo[side(c[1]), entry, from_x : from_x + 1, :]
                else:
                    line = thalo[TILE_ID[(c[0], c[1], 0)], wrapped : wrapped + 1, :]
                if c[2]:
                    entry = LEAVING[2, c[2]].index(i)
                    last = (Y - 1) if c[1] == 1 else 0
                    column = entry * chunks + from_x * halves + last // 8
                    amount = (target[c[2]] - column) % Z
                    tile = thalo[TILE_ID[c]]
                    tile = pltpu.roll(tile, amount, 1) if amount else tile
                    corner = tile[last % 8 : last % 8 + 1]
                    tile = yhalo[side(c[1]), LEAVING[1, c[1]].index(i)]
                    line = pltpu.roll(tile, turn, 1)[from_x : from_x + 1]
                    line = jnp.where(laney[0:1] == target[c[2]], corner, line)
                slab = pltpu.roll(slab, 1 if c[1] == 1 else Y - 1, 0)
                slab = jnp.where(suby == row_edge[c[1]], jnp.broadcast_to(line, (Y, Z)), slab)
            mirror = rel[PLACE[j], x * Y : (x + 1) * Y, :] if c != (0, 0, 0) else None
            if mask is not None:
                slab = jnp.where(mask, slab, mirror)
            if not inside_x:
                closed = jnp.broadcast_to(open_back[0, c[0]].astype(I32), (Y, Z))
                slab = jnp.where(closed > 0, slab, mirror)
            pv[i, x * Y : (x + 1) * Y, :] = slab
        pltpu.make_async_copy(pv.at[i], out_hbm.at[i], out_sem.at[0]).start()

    part_copy.wait()
    pltpu.make_async_copy(pv, out_hbm, out_sem.at[0]).wait()


def body(sizes, populations, solid_fraction, intersection, touch, particles, contacts, dest_code, dest_slot):
    count, X, Y, Z = populations.shape
    slots = particles.shape[4]
    touches = touch.shape[3]
    neighbours = contacts.shape[3]
    any_space = pl.BlockSpec(memory_space=pl.ANY)
    dma = pltpu.SemaphoreType.DMA
    vmem = pl.BlockSpec(memory_space=pltpu.VMEM)
    values = (
        populations.reshape(count, X * Y, Z),
        solid_fraction.reshape(X * Y, Z),
        intersection.reshape(X * Y, Z),
        touch.reshape(1, touches),
        particles.reshape(6, 1, slots),
        contacts.reshape(neighbours, 1, slots),
        dest_code.reshape(1, slots),
        dest_slot.reshape(1, slots),
    )
    handed = pl.pallas_call(
        functools.partial(kernel, sizes, (X, Y, Z)),
        out_shape=(
            pltpu.VMEM((count, X * Y, Z), F32),
            pltpu.VMEM((2, 5, Y, Z), F32),
            pltpu.VMEM((2, 5, X, Z), F32),
            pltpu.VMEM((len(TILES), 8, Z), F32),
            pltpu.VMEM((6, 1, slots), F32),
        ),
        in_specs=[pl.BlockSpec(memory_space=pltpu.HBM)] * 8,
        out_specs=(vmem,) * 5,
        scratch_shapes=[
            pltpu.VMEM((count, X * Y, Z), F32),
            pltpu.VMEM((X * Y, Z), F32),
            pltpu.VMEM((X * Y, Z), I32),
            pltpu.VMEM((1, touches), I32),
            pltpu.VMEM((neighbours, 1, slots), I32),
            pltpu.VMEM((1, slots), I32),
            pltpu.VMEM((1, slots), I32),
            pltpu.VMEM((27, 6, 1, slots), F32),
            pltpu.VMEM((6, X * Y, Z), F32),
            pltpu.VMEM((touches // LO, Z), F32),
            pltpu.VMEM((27, 4, slots), F32),
            pltpu.VMEM((27, 4, slots), F32),
            pltpu.VMEM((2, 5, X, Z), F32),
            pltpu.VMEM((2, 8, Z), F32),
            pltpu.VMEM((len(FACES), 8, slots), F32),
            pltpu.VMEM((len(FACES), 8, slots), F32),
            pltpu.VMEM((slots, 2 * touches), BF16),
            pltpu.VMEM((26 * 10 + 10 * (X + Y) + 8 * (len(TILES) + len(FACES)), Z), F32),
            pltpu.VMEM((2, 5, Y, Z), F32),
            dma((2 + X * Y // (8 * SUM_UNROLL),)),
            dma((1,)),
            dma((1,)),
            dma((1,)),
            dma((1,)),
            pltpu.SemaphoreType.REGULAR((1,)),
        ],
        compiler_params=pltpu.CompilerParams(
            collective_id=0, has_side_effects=True, vmem_limit_bytes=GRANT
        ),
    )(*[pltpu.with_memory_space_constraint(value, pltpu.HBM) for value in values])
    out, moved = pl.pallas_call(
        functools.partial(pass_kernel, sizes, (X, Y, Z)),
        out_shape=(
            jax.ShapeDtypeStruct((count, X * Y, Z), F32),
            jax.ShapeDtypeStruct((6, 1, slots), F32),
        ),
        in_specs=[vmem] * 5,
        out_specs=(any_space, any_space),
        scratch_shapes=[pltpu.VMEM((count, X * Y, Z), F32), dma((2,))],
        compiler_params=pltpu.CompilerParams(vmem_limit_bytes=GRANT),
    )(*[pltpu.with_memory_space_constraint(value, pltpu.VMEM) for value in handed])
    return (out.reshape(count, X, Y, Z), moved.reshape(1, 1, 1, 6, slots))


def solution(mesh):
    placed = (
        P(None, "gx", "gy", "gz"),
        P("gx", "gy", "gz"),
        P("gx", "gy", "gz"),
        P("gx", "gy", "gz", None),
        P("gx", "gy", "gz", None, None),
        P("gx", "gy", "gz", None, None),
        P("gx", "gy", "gz", None),
        P("gx", "gy", "gz", None),
    )
    sizes = tuple(mesh.shape[axis] for axis in ("gx", "gy", "gz"))
    return jax.shard_map(
        functools.partial(body, sizes),
        mesh=mesh,
        in_specs=placed,
        out_specs=(P(None, "gx", "gy", "gz"), P("gx", "gy", "gz", None, None)),
        check_vma=False,
    )
```
